256 devices in a mesh: dom: 128 (over z, y, x), tp: 2 (over core).
Axes of the slice: x: 4, y: 4, z: 8, core: 2. Of those that a mesh axis runs over, the one named last changes fastest.
Arguments:
- node_latent: bfloat16 [131072, 128], P('dom'), may hold values from -6 to 6
- edge_latent: bfloat16 [1048576, 128], P(('dom', 'tp')), may hold values from -6 to 6
- edge_sender: int32 [1048576], P(('dom', 'tp')), may hold values from 0 to 1535, as said below
- edge_receiver: int32 [1048576], P(('dom', 'tp')), may hold values from 0 to 1535, as said below
- edge_count: int32 [256], P(('dom', 'tp')), may hold values from 2048 to 4096, as said below
- send_index: int32 [128, 4, 128], P('dom'), may hold values from -1 to 1023, as said below
- edge_in: bfloat16 [3, 384, 128], P(None, None, 'tp'), may hold values from -0.3125 to 0.3125
- edge_out: bfloat16 [3, 128, 128], P(None, 'tp'), may hold values from -0.5 to 0.5
- node_in: bfloat16 [3, 256, 128], P(None, None, 'tp'), may hold values from -0.375 to 0.375
- node_out: bfloat16 [3, 128, 128], P(None, 'tp'), may hold values from -0.5 to 0.5
Outputs:
- node_result: bfloat16 [131072, 128], P('dom')
- edge_result: bfloat16 [1048576, 128], P(('dom', 'tp'))
The draws below stay inside these ranges and needn't reach their ends.
Inputs may be any that keep to these rules, and one draw needn't show every extreme that they name: `send_index`: entry [p, k, j] is a local node index of partition p sent to partition (p + o_k) mod 128, with o = (1, -1, 2, -2); -1 marks padding, which stands only after the live entries of a block; live entries of a block are distinct; at least half of each block is live and some block is full. `edge_sender`: an index below 1024 is an owned node of the slot's partition; index 1024 + k * 128 + j is slot j of halo block k; never a padding halo slot. `edge_receiver`: as for edge_sender. `edge_count`: some device block is full.
All inputs are finite; a program needn't handle non-finite values.
Results may differ from the reference program's by a relative error of at most 0.013.
Values may be sent and summed in bfloat16 or wider, within the bound.
A program may use at most 64 MiB of HBM per device.

```python
import jax
import jax.numpy as jnp
from jax import lax

L = 128
H = 128
NODE_DEV = 1024
SLOT = 128
PEERS = 4
LAYERS = 3
EDGE_DEV = 4096
DOMAINS = 128
SHARDS = 256
NODES = 131072
EDGES = 1048576


neighbour_offsets = (1, -1, 2, -2)


def halo_counts(key):
    counts = jax.random.randint(jax.random.fold_in(key, 11), (DOMAINS, PEERS), SLOT // 2, SLOT + 1)
    chosen = jax.random.randint(jax.random.fold_in(key, 12), (2,), 0, 1 << 20)
    counts = counts.at[chosen[0] % DOMAINS, chosen[1] % PEERS].set(SLOT)
    return counts.astype(jnp.int32)


def incoming_counts(key):
    counts = halo_counts(key)
    columns = [jnp.roll(counts[:, neighbour], offset) for neighbour, offset in enumerate(neighbour_offsets)]
    return jnp.stack(columns, axis=1)


def draw_send_index(key, part):
    counts = halo_counts(key)
    subkeys = jax.random.split(jax.random.fold_in(key, 13), DOMAINS * PEERS)
    chosen = jax.vmap(lambda subkey: jax.random.permutation(subkey, NODE_DEV)[:SLOT])(subkeys)
    chosen = chosen.reshape(DOMAINS, PEERS, SLOT)
    position = jnp.arange(SLOT, dtype=jnp.int32)[None, None, :]
    return jnp.where(position < counts[:, :, None], chosen, -1).astype(jnp.int32)


def endpoints(key, salt, halo_share):
    inbound = incoming_counts(key)
    base = jax.random.fold_in(key, salt)
    first_key, second_key, third_key, fourth_key = jax.random.split(base, 4)
    shape = (SHARDS, EDGE_DEV)
    owned_pick = jax.random.randint(first_key, shape, 0, NODE_DEV)
    block_pick = jax.random.randint(second_key, shape, 0, PEERS)
    raw_bits = jax.random.randint(third_key, shape, 0, 1 << 20)
    domain_of = (jnp.arange(SHARDS, dtype=jnp.int32) // (SHARDS // DOMAINS))[:, None]
    limit = inbound[domain_of, block_pick]
    halo_pick = NODE_DEV + block_pick * SLOT + raw_bits % limit
    use_halo = jax.random.randint(fourth_key, shape, 0, 100) < halo_share
    return jnp.where(use_halo, halo_pick, owned_pick).astype(jnp.int32).reshape(EDGES)


def draw_edge_sender(key, part):
    return endpoints(key, 21, 20)


def draw_edge_receiver(key, part):
    return endpoints(key, 22, 10)


def draw_edge_count(key, part):
    counts = jax.random.randint(jax.random.fold_in(key, 31), (SHARDS,), EDGE_DEV // 2, EDGE_DEV + 1)
    filled = jax.random.randint(jax.random.fold_in(key, 32), (), 0, SHARDS)
    return counts.at[filled].set(EDGE_DEV).astype(jnp.int32)


def block_levels(rng, dims, cuts, least, largest):
    level, own = 1.0, jax.random.fold_in(rng, 6)
    for axis_at, shards_of in cuts:
        heights = jnp.exp(jax.random.uniform(jax.random.fold_in(own, axis_at), (shards_of,), jnp.float32, least / len(cuts), largest / len(cuts)))
        level = level * jnp.repeat(heights, dims[axis_at] // shards_of).reshape([-1 if axis == axis_at else 1 for axis in range(len(dims))])
    return level


def bell_draw(rng, dims, width, bound, cuts=(), held_as=jnp.bfloat16):
    entries = jax.random.normal(rng, dims, jnp.float32) * width
    if len(cuts) > 0:
        entries = block_levels(rng, dims, cuts, -0.22, 0.18) * entries
    return jnp.clip(entries, min=-bound, max=bound).astype(held_as)


def setup_inputs(seed: int = 0) -> dict:
    arg_keys = jax.random.split(jax.random.key(seed), 11)
    node_latent = bell_draw(arg_keys[0], (NODES, L), 1.0, 6.0, ((0, 128),))
    edge_latent = bell_draw(arg_keys[1], (EDGES, L), 1.0, 6.0, ((0, 256),))
    edge_sender = draw_edge_sender(jax.random.fold_in(arg_keys[10], 71), 0)
    edge_receiver = draw_edge_receiver(jax.random.fold_in(arg_keys[10], 71), 0)
    edge_count = draw_edge_count(jax.random.fold_in(arg_keys[10], 71), 0)
    send_index = draw_send_index(jax.random.fold_in(arg_keys[10], 71), 0)
    edge_in = bell_draw(arg_keys[6], (LAYERS, 3 * L, H), (3 * L) ** -0.5, 0.3125, ((2, 2),))
    edge_out = bell_draw(arg_keys[7], (LAYERS, H, L), H ** -0.5, 0.5, ((1, 2),))
    node_in = bell_draw(arg_keys[8], (LAYERS, 2 * L, H), (2 * L) ** -0.5, 0.375, ((2, 2),))
    node_out = bell_draw(arg_keys[9], (LAYERS, H, L), H ** -0.5, 0.5, ((1, 2),))
    return {"node_latent": node_latent, "edge_latent": edge_latent, "edge_sender": edge_sender, "edge_receiver": edge_receiver, "edge_count": edge_count, "send_index": send_index, "edge_in": edge_in, "edge_out": edge_out, "node_in": node_in, "node_out": node_out}


neighbour_offsets = (1, -1, 2, -2)
norm_floor = 0.25

def layer_norm(values):
    centre = lax.optimization_barrier(jnp.mean(values, axis=-1, keepdims=True))
    centred = values - centre
    spread = lax.optimization_barrier(jnp.mean(centred * centred, axis=-1, keepdims=True))
    return centred * lax.rsqrt(spread + norm_floor)

def product(first_operand, second_operand):
    return jnp.dot(first_operand, second_operand, preferred_element_type=jnp.float32)

def reference(node_latent, edge_latent, edge_sender, edge_receiver, edge_count, send_index, edge_in, edge_out, node_in, node_out):
    feature_width = node_latent.shape[1]
    shard_count = SHARDS // DOMAINS
    extended_rows = NODE_DEV + PEERS * SLOT
    nodes_now = node_latent.reshape(DOMAINS, NODE_DEV, feature_width)
    edges_now = edge_latent.reshape(DOMAINS, shard_count * EDGE_DEV, feature_width)
    senders = edge_sender.reshape(DOMAINS, shard_count * EDGE_DEV)
    receivers = edge_receiver.reshape(DOMAINS, shard_count * EDGE_DEV)
    live_edges = (jnp.arange(EDGE_DEV, dtype=jnp.int32)[None, :] < edge_count[:, None]).reshape(DOMAINS, shard_count * EDGE_DEV)
    usable = send_index >= 0
    safe_index = jnp.where(usable, send_index, 0).astype(jnp.int32)
    domain_ids = jnp.arange(DOMAINS, dtype=jnp.int32)[:, None]
    for layer_index in range(LAYERS):
        picked = nodes_now[domain_ids[:, :, None], safe_index]
        picked = jnp.where(usable[..., None], picked, jnp.zeros((), jnp.bfloat16))
        halo_rows = jnp.stack([jnp.roll(picked[:, neighbour], offset, axis=0) for neighbour, offset in enumerate(neighbour_offsets)], axis=1)
        extended = jnp.concatenate([nodes_now, halo_rows.reshape(DOMAINS, PEERS * SLOT, feature_width)], axis=1)
        weight_in = edge_in[layer_index]
        weight_out = edge_out[layer_index]

        def edge_step(operands):
            extended_part, latent, sender_ids, receiver_ids, live_mask = operands
            linear = product(latent, weight_in[:feature_width])
            linear = linear + product(extended_part[sender_ids], weight_in[feature_width:2 * feature_width])
            linear = linear + product(extended_part[receiver_ids], weight_in[2 * feature_width:])
            edge_hidden = jnp.maximum(linear, 0.0).astype(jnp.bfloat16)
            message = jnp.where(live_mask[:, None], layer_norm(product(edge_hidden, weight_out)), 0.0).astype(jnp.bfloat16)
            message = lax.optimization_barrier(message)
            wide_message = message.astype(jnp.float32)
            renewed = (latent.astype(jnp.float32) + wide_message).astype(jnp.bfloat16)
            summed_part = jax.ops.segment_sum(wide_message, receiver_ids, num_segments=extended_rows)
            return (renewed, summed_part)
        edges_now, summed = lax.map(edge_step, (extended, edges_now, senders, receivers, live_edges))
        owned_sums = summed[:, :NODE_DEV]
        returned = summed[:, NODE_DEV:].reshape(DOMAINS, PEERS, SLOT, feature_width)
        for neighbour, offset in enumerate(neighbour_offsets):
            arrived = jnp.roll(returned[:, neighbour], -offset, axis=0)
            arrived = jnp.where(usable[:, neighbour, :, None], arrived, 0.0)
            owned_sums = owned_sums.at[domain_ids, safe_index[:, neighbour]].add(arrived)
        aggregate = owned_sums.astype(jnp.bfloat16).reshape(DOMAINS * NODE_DEV, feature_width)
        flat_nodes = nodes_now.reshape(DOMAINS * NODE_DEV, feature_width)
        first_weight = node_in[layer_index]
        linear_nodes = product(flat_nodes, first_weight[:feature_width]) + product(aggregate, first_weight[feature_width:])
        node_hidden = jnp.maximum(linear_nodes, 0.0).astype(jnp.bfloat16)
        update = layer_norm(product(node_hidden, node_out[layer_index]))
        nodes_now = (flat_nodes.astype(jnp.float32) + update).astype(jnp.bfloat16).reshape(DOMAINS, NODE_DEV, feature_width)
    return (nodes_now.reshape(NODES, feature_width), edges_now.reshape(EDGES, feature_width))
```

```python
import functools

import jax
import jax.numpy as jnp
from jax import lax
from jax.experimental import pallas as pl
from jax.experimental.pallas import tpu as pltpu
from jax.sharding import PartitionSpec as P

LAYERS = 3
OFFSETS = (1, -1, 2, -2)
NORM_FLOOR = 0.25
MESH = pl.DeviceIdType.MESH
F32 = jnp.float32
BF16 = jnp.bfloat16


def mm(a, b):
    return jnp.dot(a, b, preferred_element_type=F32)


def layer_norm(values):
    centre = jnp.mean(values, axis=-1, keepdims=True)
    centred = values - centre
    spread = jnp.mean(centred * centred, axis=-1, keepdims=True)
    return centred * lax.rsqrt(spread + NORM_FLOOR)


def hot(match):
    return jnp.where(match, 1.0, 0.0).astype(BF16)


def column(row, width):
    return jnp.transpose(jnp.broadcast_to(row, (width, width)))


def pick_half(both, high):
    return jnp.where(high, both[:, 128:], both[:, :128])


def kernel(
    doms, tile,
    x_in, e_hbm, snd, rcv, cnt, sidx, w_in, w_out, n_in, n_out,
    x_out, e_out,
    x, e, hot_s, hot_r, hot_t, code_s, code_r, acc, msg2,
    pick, pick_t, pick_hi, tab_s, tab_r, halo_sum,
    w_in_peer, n_in_peer, w_out_full, n_out_full, w_sr, w_e2, w_o2, n_in_full,
    fwd_buf, halo, ret_buf, ret, own_buf, own_peer,
    e_sem, eo_sem, w_send, w_recv, fwd_send, fwd_recv, ret_send, ret_recv,
    rel_send, rel_recv, own_send, own_recv,
):
    p = lax.axis_index("dom")
    t = lax.axis_index("tp")
    peer = (p, 1 - t)
    to = [(lax.rem(p + o + doms, doms), t) for o in OFFSETS]
    back = [(lax.rem(p - o + doms, doms), t) for o in OFFSETS]
    edges = e.shape[0]
    tiles = edges // tile
    half = tile // 2

    barrier = pltpu.get_barrier_semaphore()
    for other in to + [peer]:
        pl.semaphore_signal(barrier, inc=1, device_id=other, device_id_type=MESH)

    load_e = pltpu.make_async_copy(e_hbm, e, e_sem)
    load_e.start()

    def remote(src, dst, send, recv, device):
        return pltpu.make_async_remote_copy(
            src_ref=src, dst_ref=dst, send_sem=send, recv_sem=recv,
            device_id=device, device_id_type=MESH,
        )

    def fwd_copy(layer, k):
        return remote(fwd_buf.at[layer, k], halo.at[layer, k],
                      fwd_send.at[layer, k], fwd_recv.at[layer, k], to[k])

    def ret_copy(layer, k):
        return remote(ret_buf.at[layer, k], ret.at[layer, t, k],
                      ret_send.at[layer, k], ret_recv.at[layer, k], back[k])

    def relay_copy(layer, k):
        return remote(ret.at[layer, t, k], ret.at[layer, t, k],
                      rel_send.at[layer, k], rel_recv.at[layer, k], peer)

    def own_copy(layer):
        return remote(own_buf.at[layer], own_peer.at[layer],
                      own_send.at[layer], own_recv.at[layer], peer)

    rows64 = pl.ds(pl.multiple_of(t * 64, 64), 64)
    weight_copies = [
        remote(w_in, w_in_peer, w_send.at[0], w_recv.at[0], peer),
        remote(n_in, n_in_peer, w_send.at[1], w_recv.at[1], peer),
        remote(w_out, w_out_full.at[:, rows64, :], w_send.at[2], w_recv.at[2], peer),
        remote(n_out, n_out_full.at[:, rows64, :], w_send.at[3], w_recv.at[3], peer),
    ]

    lane = lax.broadcasted_iota(jnp.int32, (128, 128), 1)
    sub = lax.broadcasted_iota(jnp.int32, (128, 128), 0)

    for k in range(4):
        row = sidx[pl.ds(k, 1), :]
        wide = column(row, 128)
        rows = pl.ds(k * 128, 128)
        low = jnp.where(wide < 0, -1, wide & 511)
        low_row = jnp.broadcast_to(jnp.where(row < 0, -1, row & 511), (128, 128))
        pick_hi[rows, :] = jnp.where(wide >= 512, 1, 0)
        for g in range(4):
            pick[rows, g * 128 : (g + 1) * 128] = hot(low == lane + g * 128)
            pick_t[g * 128 : (g + 1) * 128, rows] = hot(low_row == sub + g * 128)

    def fill_fwd(layer):
        for k in range(4):
            rows = pl.ds(k * 128, 128)
            table = jnp.concatenate([x[0:512, :], x[512:1024, :]], axis=1)
            both = mm(pick[rows, :], table)
            fwd_buf[layer, k, :, :] = pick_half(both, pick_hi[rows, :] > 0).astype(BF16)

    x[...] = x_in[...]
    fill_fwd(0)
    pl.semaphore_wait(barrier, 5)
    for k in range(4):
        fwd_copy(0, k).start()
    for copy in weight_copies:
        copy.start()

    live = cnt[0]

    def split(row):
        own = row < 1024
        low = jnp.where(own, row & 511, 512 + (row & 255))
        high = jnp.where(own, row >> 9, (row >> 8) & 1)
        return low, high

    def build(c, carry):
        rows = pl.ds(pl.multiple_of(c * 128, 128), 128)
        low, high = split(snd[pl.ds(c, 1), :])
        both = column(low + high * 1024, 128)
        low_c = both & 1023
        code_s[rows, :] = both >> 10
        for g in range(6):
            hot_s[rows, g * 128 : (g + 1) * 128] = hot(low_c == lane + g * 128)
        low, high = split(rcv[pl.ds(c, 1), :])
        both = column(low + high * 1024, 128)
        low_c = both & 1023
        code_r[rows, :] = jnp.where(sub + c * 128 < live, both >> 10, 2)
        low_b = jnp.broadcast_to(low, (128, 128))
        for g in range(6):
            hot_r[rows, g * 128 : (g + 1) * 128] = hot(low_c == lane + g * 128)
            hot_t[g * 128 : (g + 1) * 128, rows] = hot(low_b == sub + g * 128)
        return carry

    lax.fori_loop(0, edges // 128, build, 0)

    w_out_full[:, rows64, :] = w_out[...]
    n_out_full[:, rows64, :] = n_out[...]
    for copy in weight_copies:
        copy.wait()
    first = t == 0

    def joined(mine, theirs):
        left = jnp.where(first, mine.astype(F32), theirs.astype(F32))
        right = jnp.where(first, theirs.astype(F32), mine.astype(F32))
        return jnp.concatenate([left, right], axis=-1).astype(BF16)

    w_e2[...] = jnp.zeros_like(w_e2)
    w_o2[...] = jnp.zeros_like(w_o2)
    for s in range(LAYERS):
        for part in range(3):
            rows = pl.ds(part * 128, 128)
            full = joined(w_in[s, rows, :], w_in_peer[s, rows, :])
            if part == 0:
                w_e2[s, 0:128, 0:128] = full
                w_e2[s, 128:256, 128:256] = full
            else:
                w_sr[s, :, (part - 1) * 128 : part * 128] = full
        n_in_full[s, :, :] = joined(n_in[s, :, :], n_in_peer[s, :, :])
        full = w_out_full[s, :, :]
        w_o2[s, 0:128, 0:128] = full
        w_o2[s, 128:256, 128:256] = full
    load_e.wait()

    def layer_step(s, carry):
        for h in range(2):
            proj = mm(x[h * 512 : (h + 1) * 512, :], w_sr[s, :, :]).astype(BF16)
            tab_s[0:512, h * 128 : (h + 1) * 128] = proj[:, 0:128]
            tab_r[0:512, h * 128 : (h + 1) * 128] = proj[:, 128:256]

        def owned_pass(j, c):
            start = pl.multiple_of(j * tile, tile)
            rows = pl.ds(start, tile)
            pair = jnp.concatenate(
                [e[pl.ds(start, half), :],
                 e[pl.ds(pl.multiple_of(start + half, half), half), :]], axis=1)
            lin = mm(pair, w_e2[s, :, :])
            lin = jnp.concatenate([lin[:, 0:128], lin[:, 128:256]], axis=0)
            from_s = mm(hot_s[rows, 0:512], tab_s[0:512, :])
            lin = lin + pick_half(from_s, code_s[rows, :] > 0)
            from_r = mm(hot_r[rows, 0:512], tab_r[0:512, :])
            acc[rows, :] = lin + pick_half(from_r, code_r[rows, :] == 1)
            return c

        lax.fori_loop(0, tiles, owned_pass, 0)

        for k in range(4):
            fwd_copy(s, k).wait_recv()
        for h in range(2):
            held = jnp.concatenate([halo[s, 2 * h, :, :], halo[s, 2 * h + 1, :, :]], axis=0)
            proj = mm(held, w_sr[s, :, :]).astype(BF16)
            tab_s[512:768, h * 128 : (h + 1) * 128] = proj[:, 0:128]
            tab_r[512:768, h * 128 : (h + 1) * 128] = proj[:, 128:256]
        halo_sum[...] = jnp.zeros_like(halo_sum)

        def halo_pass(j, c):
            start = pl.multiple_of(j * tile, tile)
            rows = pl.ds(start, tile)
            from_s = mm(hot_s[rows, 512:768], tab_s[512:768, :])
            from_r = mm(hot_r[rows, 512:768], tab_r[512:768, :])
            code = code_r[rows, :]
            lin = acc[rows, :] + pick_half(from_s, code_s[rows, :] > 0)
            lin = lin + pick_half(from_r, code == 1)
            hidden = jnp.maximum(lin, 0.0).astype(BF16)
            pair = jnp.concatenate([hidden[0:half, :], hidden[half:tile, :]], axis=1)
            out = mm(pair, w_o2[s, :, :])
            out = layer_norm(jnp.concatenate([out[:, 0:128], out[:, 128:256]], axis=0))
            low = jnp.where(code == 0, out, 0.0).astype(BF16)
            high = jnp.where(code == 1, out, 0.0).astype(BF16)
            both = jnp.concatenate([low, high], axis=1)
            msg2[rows, :] = both
            message = low.astype(F32) + high.astype(F32)
            e[rows, :] = (e[rows, :].astype(F32) + message).astype(BF16)
            halo_sum[...] += mm(hot_t[512:768, rows], both)

            @pl.when(s == LAYERS - 1)
            def _():
                pltpu.make_async_copy(e.at[rows, :], e_out.at[rows, :], eo_sem.at[j]).start()

            return c

        lax.fori_loop(0, tiles, halo_pass, 0)

        for k in range(4):
            rows = pl.ds((k % 2) * 128, 128)
            lanes = pl.ds((k // 2) * 128, 128)
            ret_buf[s, k, :, :] = halo_sum[rows, lanes].astype(BF16)
            ret_copy(s, k).start()

        owned = mm(hot_t[0:512, :], msg2[...]).astype(BF16)
        own_buf[s, 0:512, :] = owned[:, 0:128]
        own_buf[s, 512:1024, :] = owned[:, 128:256]
        own_copy(s).start()

        for k in range(4):
            ret_copy(s, k).wait_recv()
            relay_copy(s, k).start()
        own_copy(s).wait_recv()
        for k in range(4):
            relay_copy(s, k).wait_recv()

        back_sum = jnp.zeros((512, 256), F32)
        for source in range(2):
            for k in range(4):
                rows = pl.ds(k * 128, 128)
                high = pick_hi[rows, :] > 0
                block = ret[s, source, k, :, :].astype(F32)
                low_part = jnp.where(high, 0.0, block).astype(BF16)
                high_part = jnp.where(high, block, 0.0).astype(BF16)
                msg2[pl.ds(source * 512 + k * 128, 128), :] = jnp.concatenate(
                    [low_part, high_part], axis=1)
        back_sum = mm(pick_t[...], msg2[0:512, :]) + mm(pick_t[...], msg2[512:1024, :])
        for h in range(2):
            rows = pl.ds(h * 512, 512)
            now = x[rows, :]
            both = own_buf[s, rows, :].astype(F32) + own_peer[s, rows, :].astype(F32)
            total = (both + back_sum[:, h * 128 : (h + 1) * 128]).astype(BF16)
            lin = mm(jnp.concatenate([now, total], axis=1), n_in_full[s, :, :])
            hidden = jnp.maximum(lin, 0.0).astype(BF16)
            update = layer_norm(mm(hidden, n_out_full[s, :, :]))
            x[rows, :] = (now.astype(F32) + update).astype(BF16)

        @pl.when(s < LAYERS - 1)
        def _():
            fill_fwd(s + 1)
            for k in range(4):
                fwd_copy(s + 1, k).start()

        return carry

    lax.fori_loop(0, LAYERS, layer_step, 0)
    x_out[...] = x[...]

    for s in range(LAYERS):
        for k in range(4):
            fwd_copy(s, k).wait_send()
            ret_copy(s, k).wait_send()
            relay_copy(s, k).wait_send()
        own_copy(s).wait_send()
    for j in range(tiles):
        rows = pl.ds(j * tile, tile)
        pltpu.make_async_copy(e.at[rows, :], e_out.at[rows, :], eo_sem.at[j]).wait()


def local(
    doms,
    node_latent, edge_latent, edge_sender, edge_receiver, edge_count, send_index,
    edge_in, edge_out, node_in, node_out,
):
    edges = edge_latent.shape[0]
    tile = min(512, edges)
    tiles = edges // tile
    vmem = pl.BlockSpec(memory_space=pltpu.VMEM)
    anywhere = pl.BlockSpec(memory_space=pl.ANY)
    dma = pltpu.SemaphoreType.DMA
    scratch = [
        pltpu.VMEM((1024, 128), BF16),
        pltpu.VMEM((edges, 128), BF16),
        pltpu.VMEM((edges, 768), BF16),
        pltpu.VMEM((edges, 768), BF16),
        pltpu.VMEM((768, edges), BF16),
        pltpu.VMEM((edges, 128), jnp.int32),
        pltpu.VMEM((edges, 128), jnp.int32),
        pltpu.VMEM((edges, 128), F32),
        pltpu.VMEM((max(edges, 1024), 256), BF16),
        pltpu.VMEM((512, 512), BF16),
        pltpu.VMEM((512, 512), BF16),
        pltpu.VMEM((512, 128), jnp.int32),
        pltpu.VMEM((768, 256), BF16),
        pltpu.VMEM((768, 256), BF16),
        pltpu.VMEM((256, 256), F32),
        pltpu.VMEM(edge_in.shape, BF16),
        pltpu.VMEM(node_in.shape, BF16),
        pltpu.VMEM((LAYERS, 128, 128), BF16),
        pltpu.VMEM((LAYERS, 128, 128), BF16),
        pltpu.VMEM((LAYERS, 128, 256), BF16),
        pltpu.VMEM((LAYERS, 256, 256), BF16),
        pltpu.VMEM((LAYERS, 256, 256), BF16),
        pltpu.VMEM((LAYERS, 256, 128), BF16),
        pltpu.VMEM((LAYERS, 4, 128, 128), BF16),
        pltpu.VMEM((LAYERS, 4, 128, 128), BF16),
        pltpu.VMEM((LAYERS, 4, 128, 128), BF16),
        pltpu.VMEM((LAYERS, 2, 4, 128, 128), BF16),
        pltpu.VMEM((LAYERS, 1024, 128), BF16),
        pltpu.VMEM((LAYERS, 1024, 128), BF16),
        dma, dma((tiles,)), dma((4,)), dma((4,)),
        dma((LAYERS, 4)), dma((LAYERS, 4)), dma((LAYERS, 4)), dma((LAYERS, 4)),
        dma((LAYERS, 4)), dma((LAYERS, 4)), dma((LAYERS,)), dma((LAYERS,)),
    ]
    return pl.pallas_call(
        functools.partial(kernel, doms, tile),
        out_shape=(
            jax.ShapeDtypeStruct(node_latent.shape, BF16),
            jax.ShapeDtypeStruct(edge_latent.shape, BF16),
        ),
        in_specs=[vmem, anywhere, vmem, vmem, pl.BlockSpec(memory_space=pltpu.SMEM)]
        + [vmem] * 5,
        out_specs=(vmem, anywhere),
        scratch_shapes=scratch,
        compiler_params=pltpu.CompilerParams(
            collective_id=0, has_side_effects=True, vmem_limit_bytes=60 << 20,
        ),
    )(
        node_latent, edge_latent,
        edge_sender.reshape(-1, 128), edge_receiver.reshape(-1, 128), edge_count,
        send_index.reshape(4, 128), edge_in, edge_out, node_in, node_out,
    )


def solution(mesh):
    return jax.shard_map(
        functools.partial(local, mesh.shape["dom"]),
        mesh=mesh,
        in_specs=(
            P("dom", None),
            P(("dom", "tp"), None),
            P(("dom", "tp")),
            P(("dom", "tp")),
            P(("dom", "tp")),
            P("dom", None, None),
            P(None, None, "tp"),
            P(None, "tp", None),
            P(None, None, "tp"),
            P(None, "tp", None),
        ),
        out_specs=(P("dom", None), P(("dom", "tp"), None)),
        check_vma=False,
    )
```

```python
import functools

import jax
import jax.numpy as jnp
from jax import lax
from jax.experimental import pallas as pl
from jax.experimental.pallas import tpu as pltpu
from jax.sharding import PartitionSpec as P

LAYERS = 3
OFFSETS = (1, -1, 2, -2)
NORM_FLOOR = 0.25
MESH = pl.DeviceIdType.MESH
F32 = jnp.float32
BF16 = jnp.bfloat16
I16 = jnp.int16
I32 = jnp.int32


def mm(a, b):
    return jnp.dot(a, b, preferred_element_type=F32)


def mm_t(a, b):
    return lax.dot_general(a, b, (((1,), (1,)), ((), ())), preferred_element_type=F32)


def beside(*parts):
    return jnp.concatenate(parts, axis=1)


def below(*parts):
    return jnp.concatenate(parts, axis=0)


def layer_norm(values):
    centre = jnp.mean(values, axis=-1, keepdims=True)
    centred = values - centre
    spread = jnp.mean(centred * centred, axis=-1, keepdims=True)
    return centred * lax.rsqrt(spread + NORM_FLOOR)


def hot(match):
    return jnp.where(match, jnp.ones((), BF16), jnp.zeros((), BF16))


def column(row):
    return jnp.transpose(jnp.broadcast_to(row, (128, 128)))


def pick_half(both, high):
    return jnp.where(high, both[:, 128:], both[:, :128])


def kernel(
    doms, tile,
    x_in, e_hbm, snd, rcv, cnt, sidx, w_in, w_out, n_in, n_out,
    x_out, e_out,
    x, e, hot_s, hot_r, hot_t, code_s, code_r, acc, msg2,
    pick, pick_t, pick_hi, tab_s, tab_r,
    w_in_t, n_in_t, w_out_full, n_out_full, w_sr_t, w_e2, w_o2,
    fwd_buf, halo, ret_buf, ret, own_buf, own_peer,
    e_sem, eo_sem, w_send, w_recv, fwd_send, fwd_recv, ret_send, ret_recv,
    rel_send, rel_recv, own_send, own_recv,
):
    p = lax.axis_index("dom")
    t = lax.axis_index("tp")
    peer = (p, 1 - t)
    to = [(lax.rem(p + o + doms, doms), t) for o in OFFSETS]
    back = [(lax.rem(p - o + doms, doms), t) for o in OFFSETS]
    edges = e.shape[0]
    tiles = edges // tile
    half = tile // 2
    chunks = tile // 128

    barrier = pltpu.get_barrier_semaphore()
    for other in to + [peer]:
        pl.semaphore_signal(barrier, inc=1, device_id=other, device_id_type=MESH)

    load_e = pltpu.make_async_copy(e_hbm, e, e_sem)
    load_e.start()

    def remote(src, dst, send, recv, device):
        return pltpu.make_async_remote_copy(
            src_ref=src, dst_ref=dst, send_sem=send, recv_sem=recv,
            device_id=device, device_id_type=MESH,
        )

    def fwd_copy(layer, k):
        return remote(fwd_buf.at[layer, k], halo.at[layer, k],
                      fwd_send.at[layer, k], fwd_recv.at[layer, k], to[k])

    def ret_copy(layer, k):
        return remote(ret_buf.at[layer, k], ret.at[layer, t, k],
                      ret_send.at[layer, k], ret_recv.at[layer, k], back[k])

    def relay_copy(layer, k):
        return remote(ret.at[layer, t, k], ret.at[layer, t, k],
                      rel_send.at[layer, k], rel_recv.at[layer, k], peer)

    def own_copy(layer):
        return remote(own_buf.at[layer], own_peer.at[layer],
                      own_send.at[layer], own_recv.at[layer], peer)

    rows64 = pl.ds(pl.multiple_of(t * 64, 64), 64)
    weight_copies = [
        remote(src, dst.at[:, rows64, :], w_send.at[i], w_recv.at[i], peer)
        for i, (src, dst) in enumerate(
            [(w_in, w_in_t), (w_out, w_out_full), (n_in, n_in_t), (n_out, n_out_full)])
    ]

    lane = lax.broadcasted_iota(I32, (128, 128), 1)
    sub = lax.broadcasted_iota(I32, (128, 128), 0)
    lane16 = lane.astype(I16)
    sub16 = sub.astype(I16)

    for k in range(4):
        row = sidx[pl.ds(k, 1), :]
        wide = column(row)
        rows = pl.ds(k * 128, 128)
        low = jnp.where(wide < 0, -1, wide & 511).astype(I16)
        low_row = jnp.broadcast_to(jnp.where(row < 0, -1, row & 511), (128, 128)).astype(I16)
        pick_hi[rows, :] = jnp.where(wide >= 512, 1, 0)
        for g in range(4):
            pick[g, rows, :] = hot(low == lane16 + I16(g * 128))
            pick_t[k, g * 128 : (g + 1) * 128, :] = hot(low_row == sub16 + I16(g * 128))

    def fill_fwd(layer):
        table = beside(x[0:512, :], x[512:1024, :])
        both = mm(beside(*[pick[g, :, :] for g in range(4)]), table)
        picked = pick_half(both, pick_hi[...] > 0).astype(BF16)
        for k in range(4):
            fwd_buf[layer, k, :, :] = picked[k * 128 : (k + 1) * 128, :]

    x[...] = x_in[...]
    fill_fwd(0)
    pl.semaphore_wait(barrier, 5)
    for k in (2, 3, 0, 1):
        fwd_copy(0, k).start()
    for copy in weight_copies:
        copy.start()
    for src, dst in [(w_in, w_in_t), (w_out, w_out_full), (n_in, n_in_t), (n_out, n_out_full)]:
        dst[:, rows64, :] = src[...]
    w_e2[...] = jnp.zeros_like(w_e2)
    w_o2[...] = jnp.zeros_like(w_o2)

    live = cnt[0, 0]

    def split(row):
        own = row < 1024
        low = jnp.where(own, row & 511, 512 + (row & 255))
        high = jnp.where(own, row >> 9, (row >> 8) & 1)
        return low, high

    def build(c, carry):
        rows = pl.ds(pl.multiple_of(c * 128, 128), 128)
        low, high = split(snd[pl.ds(c, 1), :])
        both = column(low + high * 1024)
        low_c = (both & 1023).astype(I16)
        code_s[rows, :] = both >> 10
        for g in range(6):
            hot_s[g, rows, :] = hot(low_c == lane16 + I16(g * 128))
        low, high = split(rcv[pl.ds(c, 1), :])
        both = column(low + high * 1024)
        low_c = (both & 1023).astype(I16)
        code_r[rows, :] = jnp.where(sub + c * 128 < live, both >> 10, 2)
        low_b = jnp.broadcast_to(low, (128, 128)).astype(I16)
        for g in range(6):
            hot_r[g, rows, :] = hot(low_c == lane16 + I16(g * 128))
            hot_t[c, g * 128 : (g + 1) * 128, :] = hot(low_b == sub16 + I16(g * 128))
        return carry

    lax.fori_loop(0, edges // 128, build, 0)

    for copy in weight_copies:
        copy.wait()
    for s in range(LAYERS):
        full = jnp.transpose(w_in_t[s, :, 0:128].astype(F32)).astype(BF16)
        w_e2[s, 0, 0:128, :] = full
        w_e2[s, 1, 128:256, :] = full
        w_sr_t[s, 0:128, :] = w_in_t[s, :, 128:256]
        w_sr_t[s, 128:256, :] = w_in_t[s, :, 256:384]
        full = w_out_full[s, :, :]
        w_o2[s, 0, 0:128, :] = full
        w_o2[s, 1, 128:256, :] = full
    load_e.wait()

    def layer_step(s, carry):
        for h in range(2):
            proj = mm_t(x[h * 512 : (h + 1) * 512, :], w_sr_t[s, :, :]).astype(BF16)
            tab_s[h, 0:512, :] = proj[:, 0:128]
            tab_r[h, 0:512, :] = proj[:, 128:256]

        def gather(hots, tab, rows, groups, table_rows):
            return mm(beside(*[hots[g, rows, :] for g in groups]),
                      beside(tab[0, table_rows, :], tab[1, table_rows, :]))

        def owned_pass(j, c):
            start = pl.multiple_of(j * tile, tile)
            rows = pl.ds(start, tile)
            pair = beside(e[pl.ds(start, half), :],
                          e[pl.ds(pl.multiple_of(start + half, half), half), :])
            lin = mm(pair, beside(w_e2[s, 0, :, :], w_e2[s, 1, :, :]))
            lin = below(lin[:, 0:128], lin[:, 128:256])
            owned_rows = pl.ds(0, 512)
            from_s = gather(hot_s, tab_s, rows, range(4), owned_rows)
            lin = lin + pick_half(from_s, code_s[rows, :] > 0)
            from_r = gather(hot_r, tab_r, rows, range(4), owned_rows)
            acc[rows, :] = lin + pick_half(from_r, code_r[rows, :] == 1)
            return c

        lax.fori_loop(0, tiles, owned_pass, 0)

        for k in range(4):
            fwd_copy(s, k).wait_recv()
        for h in range(2):
            held = below(halo[s, 2 * h, :, :], halo[s, 2 * h + 1, :, :])
            proj = mm_t(held, w_sr_t[s, :, :]).astype(BF16)
            tab_s[h, 512:768, :] = proj[:, 0:128]
            tab_r[h, 512:768, :] = proj[:, 128:256]

        halo_rows = pl.ds(512, 256)

        def hidden_of(j):
            rows = pl.ds(j * tile, tile)
            from_s = gather(hot_s, tab_s, rows, (4, 5), halo_rows)
            from_r = gather(hot_r, tab_r, rows, (4, 5), halo_rows)
            lin = acc[rows, :] + pick_half(from_s, code_s[rows, :] > 0)
            lin = lin + pick_half(from_r, code_r[rows, :] == 1)
            return jnp.maximum(lin, 0.0).astype(BF16)

        def message_of(j, hidden):
            rows = pl.ds(j * tile, tile)
            pair = beside(hidden[0:half, :], hidden[half:tile, :])
            out = mm(pair, beside(w_o2[s, 0, :, :], w_o2[s, 1, :, :]))
            out = layer_norm(below(out[:, 0:128], out[:, 128:256]))
            code = code_r[rows, :]
            low = jnp.where(code == 0, out, 0.0).astype(BF16)
            high = jnp.where(code == 1, out, 0.0).astype(BF16)
            msg2[0, rows, :] = low
            msg2[1, rows, :] = high
            message = low.astype(F32) + high.astype(F32)
            e[rows, :] = (e[rows, :].astype(F32) + message).astype(BF16)

            @pl.when(s == LAYERS - 1)
            def _():
                pltpu.make_async_copy(e.at[rows, :], e_out.at[rows, :], eo_sem.at[j]).start()

        hidden = hidden_of(0)
        for j in range(tiles):
            later = hidden_of(j + 1) if j + 1 < tiles else None
            message_of(j, hidden)
            hidden = later

        def scatter(row_from, row_to):
            return mm(beside(*[hot_t[c, row_from:row_to, :] for c in range(edges // 128)]),
                      beside(msg2[0, 0:edges, :], msg2[1, 0:edges, :]))

        sums = scatter(512, 768).astype(BF16)
        for k in range(4):
            ret_buf[s, k, :, :] = sums[(k % 2) * 128 : (k % 2 + 1) * 128,
                                       (k // 2) * 128 : (k // 2 + 1) * 128]
        for k in (2, 3, 0, 1):
            ret_copy(s, k).start()

        owned = scatter(0, 512).astype(BF16)
        own_buf[s, 0:512, :] = owned[:, 0:128]
        own_buf[s, 512:1024, :] = owned[:, 128:256]
        own_copy(s).start()

        for k in (0, 1, 2, 3):
            ret_copy(s, k).wait_recv()
            relay_copy(s, k).start()
        own_copy(s).wait_recv()
        for k in (0, 1, 2, 3):
            relay_copy(s, k).wait_recv()

        high = pick_hi[...] > 0
        places = beside(*[pick_t[k, :, :] for k in range(4)])
        back_sum = None
        for source in range(2):
            block = below(*[ret[s, source, k, :, :] for k in range(4)]).astype(F32)
            both = beside(jnp.where(high, 0.0, block), jnp.where(high, block, 0.0)).astype(BF16)
            part = mm(places, both)
            back_sum = part if back_sum is None else back_sum + part
        for h in range(2):
            rows = pl.ds(h * 512, 512)
            now = x[rows, :]
            both = own_buf[s, rows, :].astype(F32) + own_peer[s, rows, :].astype(F32)
            total = (both + back_sum[:, h * 128 : (h + 1) * 128]).astype(BF16)
            hidden = jnp.maximum(mm_t(beside(now, total), n_in_t[s, :, :]), 0.0).astype(BF16)
            update = layer_norm(mm(hidden, n_out_full[s, :, :]))
            x[rows, :] = (now.astype(F32) + update).astype(BF16)

        @pl.when(s < LAYERS - 1)
        def _():
            fill_fwd(s + 1)
            for k in (2, 3, 0, 1):
                fwd_copy(s + 1, k).start()

        return carry

    lax.fori_loop(0, LAYERS, layer_step, 0)
    x_out[...] = x[...]

    for s in range(LAYERS):
        for k in range(4):
            fwd_copy(s, k).wait_send()
            ret_copy(s, k).wait_send()
            relay_copy(s, k).wait_send()
        own_copy(s).wait_send()
    for j in range(tiles):
        rows = pl.ds(j * tile, tile)
        pltpu.make_async_copy(e.at[rows, :], e_out.at[rows, :], eo_sem.at[j]).wait()


def local(
    doms,
    node_latent, edge_latent, edge_sender, edge_receiver, edge_count, send_index,
    edge_in, edge_out, node_in, node_out,
):
    edges = edge_latent.shape[0]
    tile = min(512, edges)
    tiles = edges // tile
    vmem = pl.BlockSpec(memory_space=pltpu.VMEM)
    anywhere = pl.BlockSpec(memory_space=pl.ANY)
    dma = pltpu.SemaphoreType.DMA
    scratch = [
        pltpu.VMEM((1024, 128), BF16),
        pltpu.VMEM((edges, 128), BF16),
        pltpu.VMEM((6, edges, 128), BF16),
        pltpu.VMEM((6, edges, 128), BF16),
        pltpu.VMEM((edges // 128, 768, 128), BF16),
        pltpu.VMEM((edges, 128), I32),
        pltpu.VMEM((edges, 128), I32),
        pltpu.VMEM((edges, 128), F32),
        pltpu.VMEM((2, edges, 128), BF16),
        pltpu.VMEM((4, 512, 128), BF16),
        pltpu.VMEM((4, 512, 128), BF16),
        pltpu.VMEM((512, 128), I32),
        pltpu.VMEM((2, 768, 128), BF16),
        pltpu.VMEM((2, 768, 128), BF16),
        pltpu.VMEM((LAYERS, 128, 384), BF16),
        pltpu.VMEM((LAYERS, 128, 256), BF16),
        pltpu.VMEM((LAYERS, 128, 128), BF16),
        pltpu.VMEM((LAYERS, 128, 128), BF16),
        pltpu.VMEM((LAYERS, 256, 128), BF16),
        pltpu.VMEM((LAYERS, 2, 256, 128), BF16),
        pltpu.VMEM((LAYERS, 2, 256, 128), BF16),
        pltpu.VMEM((LAYERS, 4, 128, 128), BF16),
        pltpu.VMEM((LAYERS, 4, 128, 128), BF16),
        pltpu.VMEM((LAYERS, 4, 128, 128), BF16),
        pltpu.VMEM((LAYERS, 2, 4, 128, 128), BF16),
        pltpu.VMEM((LAYERS, 1024, 128), BF16),
        pltpu.VMEM((LAYERS, 1024, 128), BF16),
        dma, dma((tiles,)), dma((4,)), dma((4,)),
        dma((LAYERS, 4)), dma((LAYERS, 4)), dma((LAYERS, 4)), dma((LAYERS, 4)),
        dma((LAYERS, 4)), dma((LAYERS, 4)), dma((LAYERS,)), dma((LAYERS,)),
    ]
    return pl.pallas_call(
        functools.partial(kernel, doms, tile),
        out_shape=(
            jax.ShapeDtypeStruct(node_latent.shape, BF16),
            jax.ShapeDtypeStruct(edge_latent.shape, BF16),
        ),
        in_specs=[vmem, anywhere, vmem, vmem, pl.BlockSpec(memory_space=pltpu.SMEM)]
        + [vmem] * 5,
        out_specs=(vmem, anywhere),
        scratch_shapes=scratch,
        compiler_params=pltpu.CompilerParams(
            collective_id=0, has_side_effects=True, vmem_limit_bytes=60 << 20,
        ),
    )(
        node_latent, edge_latent,
        edge_sender.reshape(-1, 128), edge_receiver.reshape(-1, 128),
        edge_count.reshape(1, 1), send_index.reshape(4, 128),
        jnp.swapaxes(edge_in, 1, 2), edge_out, jnp.swapaxes(node_in, 1, 2), node_out,
    )


def solution(mesh):
    return jax.shard_map(
        functools.partial(local, mesh.shape["dom"]),
        mesh=mesh,
        in_specs=(
            P("dom", None),
            P(("dom", "tp"), None),
            P(("dom", "tp")),
            P(("dom", "tp")),
            P(("dom", "tp")),
            P("dom", None, None),
            P(None, None, "tp"),
            P(None, "tp", None),
            P(None, None, "tp"),
            P(None, "tp", None),
        ),
        out_specs=(P("dom", None), P(("dom", "tp"), None)),
        check_vma=False,
    )
```

```python
import functools

import jax
import jax.numpy as jnp
from jax import lax
from jax.experimental import pallas as pl
from jax.experimental.pallas import tpu as pltpu
from jax.sharding import PartitionSpec as P

LAYERS = 3
OFFSETS = (1, -1, 2, -2)
NORM_FLOOR = 0.25
MESH = pl.DeviceIdType.MESH
F32 = jnp.float32
BF16 = jnp.bfloat16
I16 = jnp.int16
I32 = jnp.int32


def mm(a, b):
    return jnp.dot(a, b, preferred_element_type=F32)


def mm_t(a, b):
    return lax.dot_general(a, b, (((1,), (1,)), ((), ())), preferred_element_type=F32)


def beside(*parts):
    return jnp.concatenate(parts, axis=1)


def below(*parts):
    return jnp.concatenate(parts, axis=0)


def layer_norm(values):
    centre = jnp.mean(values, axis=-1, keepdims=True)
    centred = values - centre
    spread = jnp.mean(centred * centred, axis=-1, keepdims=True)
    return centred * lax.rsqrt(spread + NORM_FLOOR)


def hot(match):
    return jnp.where(match, jnp.ones((), BF16), jnp.zeros((), BF16))


def column(row):
    return jnp.transpose(jnp.broadcast_to(row, (128, 128)))


def pick_half(both, high):
    return jnp.where(high, both[:, 128:], both[:, :128])


def kernel(
    doms, tile,
    x_in, e_hbm, snd, rcv, cnt, sidx, w_in, w_out, n_in, n_out,
    x, e,
    hot_s, hot_r, hot_t, code, masks, acc, msg2,
    pick, pick_t, pick_hi, tab_s, tab_r,
    w_in_t, n_in_t, w_out_full, n_out_full, w_sr_t, w_e2, w_o2,
    fwd_buf, halo, ret_buf, ret, own_buf, own_peer,
    e_sem, w_send, w_recv, fwd_send, fwd_recv, ret_send, ret_recv,
    rel_send, rel_recv, own_send, own_recv,
):
    p = lax.axis_index("dom")
    t = lax.axis_index("tp")
    peer = (p, 1 - t)
    to = [(lax.rem(p + o + doms, doms), t) for o in OFFSETS]
    back = [(lax.rem(p - o + doms, doms), t) for o in OFFSETS]
    edges = e.shape[0]
    tiles = edges // tile
    half = tile // 2
    chunks = tile // 128

    barrier = pltpu.get_barrier_semaphore()
    for other in to + [peer]:
        pl.semaphore_signal(barrier, inc=1, device_id=other, device_id_type=MESH)

    load_e = pltpu.make_async_copy(e_hbm, e, e_sem)
    load_e.start()

    def remote(src, dst, send, recv, device):
        return pltpu.make_async_remote_copy(
            src_ref=src, dst_ref=dst, send_sem=send, recv_sem=recv,
            device_id=device, device_id_type=MESH,
        )

    def fwd_copy(layer, k):
        return remote(fwd_buf.at[layer, k], halo.at[layer, k],
                      fwd_send.at[layer, k], fwd_recv.at[layer, k], to[k])

    def ret_copy(layer, k):
        return remote(ret_buf.at[layer, k], ret.at[layer, t, k],
                      ret_send.at[layer, k], ret_recv.at[layer, k], back[k])

    def relay_copy(layer, k):
        return remote(ret.at[layer, t, k], ret.at[layer, t, k],
                      rel_send.at[layer, k], rel_recv.at[layer, k], peer)

    def own_copy(layer):
        return remote(own_buf.at[layer], own_peer.at[layer],
                      own_send.at[layer], own_recv.at[layer], peer)

    rows64 = pl.ds(pl.multiple_of(t * 64, 64), 64)
    weight_copies = [
        remote(src, dst.at[:, rows64, :], w_send.at[i], w_recv.at[i], peer)
        for i, (src, dst) in enumerate(
            [(w_in, w_in_t), (w_out, w_out_full), (n_in, n_in_t), (n_out, n_out_full)])
    ]

    lane = lax.broadcasted_iota(I32, (128, 128), 1)
    sub = lax.broadcasted_iota(I32, (128, 128), 0)
    lane16 = lax.broadcasted_iota(I32, (16, 128), 1).astype(I16)
    sub16 = lax.broadcasted_iota(I32, (16, 128), 0).astype(I16)
    lane_of = [lane16 + I16(g * 128) for g in range(6)]

    def hot_columns(ref, groups, start, low):
        for i in range(8):
            part = low[i * 16 : (i + 1) * 16, :]
            for g in range(groups):
                ref[g, pl.ds(start + i * 16, 16), :] = hot(part == lane_of[g])

    def hot_rows(ref, c, count, low_row):
        wide = jnp.broadcast_to(low_row, (16, 128)).astype(I16)
        for i in range(count // 16):
            ref[c, i * 16 : (i + 1) * 16, :] = hot(wide - I16(i * 16) == sub16)

    for k in range(4):
        row = sidx[pl.ds(k, 1), :]
        wide = column(row)
        rows = pl.ds(k * 128, 128)
        low = jnp.where(wide < 0, -1, wide & 511).astype(I16)
        pick_hi[rows, :] = jnp.where(wide >= 512, 1, 0)
        hot_columns(pick, 4, k * 128, low)
        hot_rows(pick_t, k, 512, jnp.where(row < 0, -1, row & 511))

    def fill_fwd(layer):
        table = beside(x[0:512, :], x[512:1024, :])
        both = mm(beside(*[pick[g, :, :] for g in range(4)]), table)
        picked = pick_half(both, pick_hi[...] > 0).astype(BF16)
        for k in range(4):
            fwd_buf[layer, k, :, :] = picked[k * 128 : (k + 1) * 128, :]

    x[...] = x_in[...]
    fill_fwd(0)
    pl.semaphore_wait(barrier, 5)
    for k in (2, 3, 0, 1):
        fwd_copy(0, k).start()
    for copy in weight_copies:
        copy.start()
    for src, dst in [(w_in, w_in_t), (w_out, w_out_full), (n_in, n_in_t), (n_out, n_out_full)]:
        dst[:, rows64, :] = src[...]
    w_e2[...] = jnp.zeros_like(w_e2)
    w_o2[...] = jnp.zeros_like(w_o2)

    live = cnt[0, 0]

    def split(row):
        own = row < 1024
        low = jnp.where(own, row & 511, 512 + (row & 255))
        high = jnp.where(own, row >> 9, (row >> 8) & 1)
        return low, high

    def build(c, carry):
        start = pl.multiple_of(c * 128, 128)
        rows = pl.ds(start, 128)
        low, high = split(snd[pl.ds(c, 1), :])
        low_r, high_r = split(rcv[pl.ds(c, 1), :])
        hot_rows(hot_t, c, 768, low_r)
        both = column(low + high * 1024)
        both_r = column(low_r + high_r * 1024)
        hot_columns(hot_s, 6, start, (both & 1023).astype(I16))
        hot_columns(hot_r, 6, start, (both_r & 1023).astype(I16))
        high = both >> 10
        high_r = both_r >> 10
        code[rows, :] = high + 2 * high_r
        place = jnp.where(sub + start < live, high_r, 2)
        masks[0, rows, :] = jnp.where(place == 0, 1.0, 0.0).astype(BF16)
        masks[1, rows, :] = jnp.where(place == 1, 1.0, 0.0).astype(BF16)
        return carry

    lax.fori_loop(0, edges // 128, build, 0)

    for copy in weight_copies:
        copy.wait()
    for s in range(LAYERS):
        full = jnp.transpose(w_in_t[s, :, 0:128].astype(F32)).astype(BF16)
        w_e2[s, 0, 0:128, :] = full
        w_e2[s, 1, 128:256, :] = full
        w_sr_t[s, 0:128, :] = w_in_t[s, :, 128:256]
        w_sr_t[s, 128:256, :] = w_in_t[s, :, 256:384]
        full = w_out_full[s, :, :]
        w_o2[s, 0, 0:128, :] = full
        w_o2[s, 1, 128:256, :] = full
    load_e.wait()

    def layer_step(s, carry):
        for h in range(2):
            proj = mm_t(x[h * 512 : (h + 1) * 512, :], w_sr_t[s, :, :]).astype(BF16)
            tab_s[h, 0:512, :] = proj[:, 0:128]
            tab_r[h, 0:512, :] = proj[:, 128:256]

        def gather(hots, tab, rows, groups, table_rows):
            return mm(beside(*[hots[g, rows, :] for g in groups]),
                      beside(tab[0, table_rows, :], tab[1, table_rows, :]))

        def with_picked(lin, from_s, from_r, rows):
            held = code[rows, :]
            lin = lin + pick_half(from_s, (held & 1) > 0)
            return lin + pick_half(from_r, held > 1)

        owned_rows = pl.ds(0, 512)
        for j in range(tiles):
            rows = pl.ds(j * tile, tile)
            pair = beside(e[pl.ds(j * tile, half), :], e[pl.ds(j * tile + half, half), :])
            lin = mm(pair, beside(w_e2[s, 0, :, :], w_e2[s, 1, :, :]))
            lin = below(lin[:, 0:128], lin[:, 128:256])
            from_s = gather(hot_s, tab_s, rows, range(4), owned_rows)
            from_r = gather(hot_r, tab_r, rows, range(4), owned_rows)
            acc[rows, :] = with_picked(lin, from_s, from_r, rows)

        for k in range(4):
            fwd_copy(s, k).wait_recv()
        for h in range(2):
            held = below(halo[s, 2 * h, :, :], halo[s, 2 * h + 1, :, :])
            proj = mm_t(held, w_sr_t[s, :, :]).astype(BF16)
            tab_s[h, 512:768, :] = proj[:, 0:128]
            tab_r[h, 512:768, :] = proj[:, 128:256]

        halo_rows = pl.ds(512, 256)

        def hidden_of(j):
            rows = pl.ds(j * tile, tile)
            from_s = gather(hot_s, tab_s, rows, (4, 5), halo_rows)
            from_r = gather(hot_r, tab_r, rows, (4, 5), halo_rows)
            lin = with_picked(acc[rows, :], from_s, from_r, rows)
            return jnp.maximum(lin, 0.0).astype(BF16)

        def message_of(j, hidden):
            rows = pl.ds(j * tile, tile)
            pair = beside(hidden[0:half, :], hidden[half:tile, :])
            out = mm(pair, beside(w_o2[s, 0, :, :], w_o2[s, 1, :, :]))
            out = layer_norm(below(out[:, 0:128], out[:, 128:256]))
            out = out.astype(BF16)
            low = out * masks[0, rows, :]
            high = out * masks[1, rows, :]
            msg2[0, rows, :] = low
            msg2[1, rows, :] = high
            e[rows, :] = e[rows, :] + (low + high)

        hidden = hidden_of(0)
        for j in range(tiles):
            later = hidden_of(j + 1) if j + 1 < tiles else None
            message_of(j, hidden)
            hidden = later

        def scatter(row_from, row_to):
            return mm(beside(*[hot_t[c, row_from:row_to, :] for c in range(edges // 128)]),
                      beside(msg2[0, 0:edges, :], msg2[1, 0:edges, :])).astype(BF16)

        for i in range(2):
            sums = scatter(512 + i * 128, 640 + i * 128)
            ret_buf[s, i, :, :] = sums[:, 0:128]
            ret_buf[s, 2 + i, :, :] = sums[:, 128:256]
        for k in (2, 3, 0, 1):
            ret_copy(s, k).start()

        for i in range(4):
            owned = scatter(i * 128, (i + 1) * 128)
            own_buf[s, i * 128 : (i + 1) * 128, :] = owned[:, 0:128]
            own_buf[s, 512 + i * 128 : 512 + (i + 1) * 128, :] = owned[:, 128:256]
        own_copy(s).start()

        for k in (0, 1, 2, 3):
            ret_copy(s, k).wait_recv()
            relay_copy(s, k).start()
        own_copy(s).wait_recv()
        for k in (0, 1, 2, 3):
            relay_copy(s, k).wait_recv()

        high = pick_hi[...] > 0
        places = beside(*[pick_t[k, :, :] for k in range(4)])
        back_sum = None
        for source in range(2):
            block = below(*[ret[s, source, k, :, :] for k in range(4)]).astype(F32)
            both = beside(jnp.where(high, 0.0, block), jnp.where(high, block, 0.0)).astype(BF16)
            part = mm(places, both)
            back_sum = part if back_sum is None else back_sum + part
        for h in range(2):
            rows = pl.ds(h * 512, 512)
            now = x[rows, :]
            both = own_buf[s, rows, :].astype(F32) + own_peer[s, rows, :].astype(F32)
            total = (both + back_sum[:, h * 128 : (h + 1) * 128]).astype(BF16)
            hidden = jnp.maximum(mm_t(beside(now, total), n_in_t[s, :, :]), 0.0).astype(BF16)
            update = layer_norm(mm(hidden, n_out_full[s, :, :]))
            x[rows, :] = (now.astype(F32) + update).astype(BF16)

        @pl.when(s < LAYERS - 1)
        def _():
            fill_fwd(s + 1)
            for k in (2, 3, 0, 1):
                fwd_copy(s + 1, k).start()

        return carry

    lax.fori_loop(0, LAYERS, layer_step, 0)

    for s in range(LAYERS):
        for k in range(4):
            fwd_copy(s, k).wait_send()
            ret_copy(s, k).wait_send()
            relay_copy(s, k).wait_send()
        own_copy(s).wait_send()


def local(
    doms,
    node_latent, edge_latent, edge_sender, edge_receiver, edge_count, send_index,
    edge_in, edge_out, node_in, node_out,
):
    edges = edge_latent.shape[0]
    tile = min(512, edges)
    tiles = edges // tile
    vmem = pl.BlockSpec(memory_space=pltpu.VMEM)
    hbm = pl.BlockSpec(memory_space=pltpu.HBM)
    dma = pltpu.SemaphoreType.DMA
    scratch = [
        pltpu.VMEM((6, edges, 128), BF16),
        pltpu.VMEM((6, edges, 128), BF16),
        pltpu.VMEM((edges // 128, 768, 128), BF16),
        pltpu.VMEM((edges, 128), I32),
        pltpu.VMEM((2, edges, 128), BF16),
        pltpu.VMEM((edges, 128), F32),
        pltpu.VMEM((2, edges, 128), BF16),
        pltpu.VMEM((4, 512, 128), BF16),
        pltpu.VMEM((4, 512, 128), BF16),
        pltpu.VMEM((512, 128), I32),
        pltpu.VMEM((2, 768, 128), BF16),
        pltpu.VMEM((2, 768, 128), BF16),
        pltpu.VMEM((LAYERS, 128, 384), BF16),
        pltpu.VMEM((LAYERS, 128, 256), BF16),
        pltpu.VMEM((LAYERS, 128, 128), BF16),
        pltpu.VMEM((LAYERS, 128, 128), BF16),
        pltpu.VMEM((LAYERS, 256, 128), BF16),
        pltpu.VMEM((LAYERS, 2, 256, 128), BF16),
        pltpu.VMEM((LAYERS, 2, 256, 128), BF16),
        pltpu.VMEM((LAYERS, 4, 128, 128), BF16),
        pltpu.VMEM((LAYERS, 4, 128, 128), BF16),
        pltpu.VMEM((LAYERS, 4, 128, 128), BF16),
        pltpu.VMEM((LAYERS, 2, 4, 128, 128), BF16),
        pltpu.VMEM((LAYERS, 1024, 128), BF16),
        pltpu.VMEM((LAYERS, 1024, 128), BF16),
        dma, dma((4,)), dma((4,)),
        dma((LAYERS, 4)), dma((LAYERS, 4)), dma((LAYERS, 4)), dma((LAYERS, 4)),
        dma((LAYERS, 4)), dma((LAYERS, 4)), dma((LAYERS,)), dma((LAYERS,)),
    ]
    return pl.pallas_call(
        functools.partial(kernel, doms, tile),
        out_shape=(
            pltpu.VMEM(node_latent.shape, BF16),
            pltpu.VMEM(edge_latent.shape, BF16),
        ),
        in_specs=[vmem, hbm, vmem, vmem, pl.BlockSpec(memory_space=pltpu.SMEM)]
        + [vmem] * 5,
        out_specs=(vmem, vmem),
        scratch_shapes=scratch,
        compiler_params=pltpu.CompilerParams(
            collective_id=0, has_side_effects=True, vmem_limit_bytes=65700000,
        ),
    )(
        node_latent, edge_latent,
        edge_sender.reshape(-1, 128), edge_receiver.reshape(-1, 128),
        edge_count.reshape(1, 1), send_index.reshape(4, 128),
        jnp.swapaxes(edge_in, 1, 2), edge_out, jnp.swapaxes(node_in, 1, 2), node_out,
    )


def solution(mesh):
    return jax.shard_map(
        functools.partial(local, mesh.shape["dom"]),
        mesh=mesh,
        in_specs=(
            P("dom", None),
            P(("dom", "tp"), None),
            P(("dom", "tp")),
            P(("dom", "tp")),
            P(("dom", "tp")),
            P("dom", None, None),
            P(None, None, "tp"),
            P(None, "tp", None),
            P(None, None, "tp"),
            P(None, "tp", None),
        ),
        out_specs=(P("dom", None), P(("dom", "tp"), None)),
        check_vma=False,
    )
```

```python
import functools

import jax
import jax.numpy as jnp
from jax import lax
from jax.experimental import pallas as pl
from jax.experimental.pallas import tpu as pltpu
from jax.sharding import PartitionSpec as P

LAYERS = 3
OFFSETS = (1, -1, 2, -2)
NORM_FLOOR = 0.25
MESH = pl.DeviceIdType.MESH
F32 = jnp.float32
BF16 = jnp.bfloat16
I16 = jnp.int16
I32 = jnp.int32


def mm(a, b):
    return jnp.dot(a, b, preferred_element_type=F32)


def mm_t(a, b):
    return lax.dot_general(a, b, (((1,), (1,)), ((), ())), preferred_element_type=F32)


def beside(*parts):
    return jnp.concatenate(parts, axis=1)


def below(*parts):
    return jnp.concatenate(parts, axis=0)


def layer_norm(values):
    centre = jnp.mean(values, axis=-1, keepdims=True)
    centred = values - centre
    spread = jnp.mean(centred * centred, axis=-1, keepdims=True)
    return centred * lax.rsqrt(spread + NORM_FLOOR)


def hot(match):
    return jnp.where(match, jnp.ones((), BF16), jnp.zeros((), BF16))


def column(row):
    return jnp.transpose(jnp.broadcast_to(row, (128, 128)))


def pick_half(both, high):
    return jnp.where(high, both[:, 128:], both[:, :128])


def kernel(
    doms, tile,
    x_in, e_hbm, snd, rcv, cnt, sidx, w_in, w_out, n_in, n_out,
    x, e,
    hot_s, hot_r, hot_t, code, acc, msg2,
    pick, pick_t, pick_hi, tab_s, tab_r, back_sum, own_sum, own_lin,
    w_in_t, n_in_t, w_out_full, n_out_full, w_sr_t, w_e2, w_o2,
    fwd_buf, halo, ret_buf, ret, own_buf, own_peer,
    e_sem, w_send, w_recv, fwd_send, fwd_recv, ret_send, ret_recv,
    rel_send, rel_recv, own_send, own_recv,
):
    p = lax.axis_index("dom")
    t = lax.axis_index("tp")
    peer = (p, 1 - t)
    to = [(lax.rem(p + o + doms, doms), 1 - t) for o in OFFSETS]
    back = [(lax.rem(p - o + doms, doms), 1 - t) for o in OFFSETS]
    edges = e.shape[0]
    tiles = edges // tile
    half = tile // 2
    chunks = tile // 128

    barrier = pltpu.get_barrier_semaphore()
    for other in to + [peer]:
        pl.semaphore_signal(barrier, inc=1, device_id=other, device_id_type=MESH)

    load_e = pltpu.make_async_copy(e_hbm, e, e_sem)
    load_e.start()

    def remote(src, dst, send, recv, device):
        return pltpu.make_async_remote_copy(
            src_ref=src, dst_ref=dst, send_sem=send, recv_sem=recv,
            device_id=device, device_id_type=MESH,
        )

    def fwd_copy(layer, k):
        return remote(fwd_buf.at[layer, k], halo.at[layer, k],
                      fwd_send.at[layer, k], fwd_recv.at[layer, k], to[k])

    def ret_copy(layer, k):
        return remote(ret_buf.at[layer, k], ret.at[layer, 1 - t, k],
                      ret_send.at[layer, k], ret_recv.at[layer, k], back[k])

    def relay_copy(layer, k):
        return remote(ret.at[layer, t, k], ret.at[layer, t, k],
                      rel_send.at[layer, k], rel_recv.at[layer, k], peer)

    def own_copy(layer):
        return remote(own_buf.at[layer], own_peer.at[layer],
                      own_send.at[layer], own_recv.at[layer], peer)

    rows64 = pl.ds(pl.multiple_of(t * 64, 64), 64)
    weight_copies = [
        remote(src, dst.at[:, rows64, :], w_send.at[i], w_recv.at[i], peer)
        for i, (src, dst) in enumerate(
            [(w_in, w_in_t), (w_out, w_out_full), (n_in, n_in_t), (n_out, n_out_full)])
    ]

    lane = lax.broadcasted_iota(I32, (128, 128), 1)
    sub = lax.broadcasted_iota(I32, (128, 128), 0)
    sub16 = lax.broadcasted_iota(I32, (16, 128), 0).astype(I16)
    lane_of = [lax.broadcasted_iota(I32, (16, 128), 1) + g * 128 for g in range(6)]

    def hot_columns(ref, groups, start, low):
        for i in range(8):
            part = low[i * 16 : (i + 1) * 16, :]
            for g in range(groups):
                ref[g, pl.ds(start + i * 16, 16), :] = jnp.where(
                    part == lane_of[g], 1.0, 0.0).astype(BF16)

    def hot_rows(ref, c, row_from, row_to, low_row):
        wide = jnp.broadcast_to(low_row, (16, 128)).astype(I16)
        for i in range(row_from // 16, row_to // 16):
            ref[c, i * 16 : (i + 1) * 16, :] = hot(wide - I16(i * 16) == sub16)

    for k in range(4):
        row = sidx[pl.ds(k, 1), :]
        wide = column(row)
        rows = pl.ds(k * 128, 128)
        low = jnp.where(wide < 0, -1, wide & 511)
        pick_hi[rows, :] = jnp.where(wide >= 512, 1, 0)
        hot_columns(pick, 4, k * 128, low)

    def fill_fwd(layer):
        table = beside(x[0:512, :], x[512:1024, :])
        both = mm(beside(*[pick[g, :, :] for g in range(4)]), table)
        picked = pick_half(both, pick_hi[...] > 0).astype(BF16)
        for k in range(4):
            fwd_buf[layer, k, :, :] = picked[k * 128 : (k + 1) * 128, :]

    x[...] = x_in[...]
    fill_fwd(0)
    for src, dst in [(w_in, w_in_t), (w_out, w_out_full), (n_in, n_in_t), (n_out, n_out_full)]:
        dst[:, rows64, :] = src[...]
    w_e2[...] = jnp.zeros_like(w_e2)
    w_o2[...] = jnp.zeros_like(w_o2)
    pl.semaphore_wait(barrier, 5)
    for k in range(4):
        fwd_copy(0, k).start()
    for copy in weight_copies:
        copy.start()

    live = cnt[0, 0]

    def split(row):
        own = row < 1024
        low = jnp.where(own, row & 511, 512 + (row & 255))
        high = jnp.where(own, row >> 9, (row >> 8) & 1)
        return low, high

    def build_one(c):
        start = pl.multiple_of(c * 128, 128)
        rows = pl.ds(start, 128)
        low, high = split(snd[pl.ds(c, 1), :])
        low_r, high_r = split(rcv[pl.ds(c, 1), :])
        hot_rows(hot_t, c, 512, 768, low_r)
        both = column(low + high * 1024)
        both_r = column(low_r + high_r * 1024)
        hot_columns(hot_s, 6, start, both & 1023)
        hot_columns(hot_r, 6, start, both_r & 1023)
        alive = sub + start < live
        held = jnp.where(both_r >= 1024, jnp.where(alive, 6, 4), jnp.where(alive, 0, 2))
        code[rows, :] = held + (both >> 10)

    def build(i, carry):
        for c in range(4):
            build_one(i * 4 + c)
        return carry

    lax.fori_loop(0, edges // 512, build, 0)

    for copy in weight_copies:
        copy.wait()
    for s in range(LAYERS):
        full = jnp.transpose(w_in_t[s, :, 0:128].astype(F32)).astype(BF16)
        w_e2[s, 0, 0:128, :] = full
        w_e2[s, 1, 128:256, :] = full
        w_sr_t[s, 0:128, :] = w_in_t[s, :, 128:256]
        w_sr_t[s, 128:256, :] = w_in_t[s, :, 256:384]
        full = w_out_full[s, :, :]
        w_o2[s, 0, 0:128, :] = full
        w_o2[s, 1, 128:256, :] = full
    load_e.wait()

    def layer_step(s, carry):
        for h in range(2):
            proj = mm_t(x[h * 512 : (h + 1) * 512, :], w_sr_t[s, :, :]).astype(BF16)
            tab_s[h, 0:512, :] = proj[:, 0:128]
            tab_r[h, 0:512, :] = proj[:, 128:256]

        def gather(hots, tab, rows, groups, table_rows):
            return mm(beside(*[hots[g, rows, :] for g in groups]),
                      beside(tab[0, table_rows, :], tab[1, table_rows, :]))

        def with_picked(lin, from_s, from_r, rows):
            held = code[rows, :]
            lin = lin + pick_half(from_s, (held & 1) > 0)
            return lin + pick_half(from_r, held >= 4)

        owned_rows = pl.ds(0, 512)
        for j in range(tiles):
            rows = pl.ds(j * tile, tile)
            pair = beside(e[pl.ds(j * tile, half), :], e[pl.ds(j * tile + half, half), :])
            lin = mm(pair, beside(w_e2[s, 0, :, :], w_e2[s, 1, :, :]))
            lin = below(lin[:, 0:128], lin[:, 128:256])
            from_s = gather(hot_s, tab_s, rows, range(4), owned_rows)
            from_r = gather(hot_r, tab_r, rows, range(4), owned_rows)
            acc[rows, :] = with_picked(lin, from_s, from_r, rows)

        for k in range(4):
            fwd_copy(s, k).wait_recv()
        for h in range(2):
            held = below(halo[s, 2 * h, :, :], halo[s, 2 * h + 1, :, :])
            proj = mm_t(held, w_sr_t[s, :, :]).astype(BF16)
            tab_s[h, 512:768, :] = proj[:, 0:128]
            tab_r[h, 512:768, :] = proj[:, 128:256]

        halo_rows = pl.ds(512, 256)

        def hidden_of(j):
            rows = pl.ds(j * tile, tile)
            from_s = gather(hot_s, tab_s, rows, (4, 5), halo_rows)
            from_r = gather(hot_r, tab_r, rows, (4, 5), halo_rows)
            lin = with_picked(acc[rows, :], from_s, from_r, rows)
            return jnp.maximum(lin, 0.0).astype(BF16)

        def message_of(j, hidden):
            rows = pl.ds(j * tile, tile)
            pair = beside(hidden[0:half, :], hidden[half:tile, :])
            out = mm(pair, beside(w_o2[s, 0, :, :], w_o2[s, 1, :, :]))
            out = layer_norm(below(out[:, 0:128], out[:, 128:256]))
            held = code[rows, :]
            msg2[0, rows, :] = jnp.where(held < 2, out, 0.0).astype(BF16)
            msg2[1, rows, :] = jnp.where(held >= 6, out, 0.0).astype(BF16)

        hidden = hidden_of(0)
        for j in range(tiles):
            later = hidden_of(j + 1) if j + 1 < tiles else None
            message_of(j, hidden)
            hidden = later

        def scatter(row_from, row_to):
            return mm(beside(*[hot_t[c, row_from:row_to, :] for c in range(edges // 128)]),
                      beside(msg2[0, 0:edges, :], msg2[1, 0:edges, :])).astype(BF16)

        for i in range(2):
            sums = scatter(512 + i * 128, 640 + i * 128)
            ret_buf[s, i, :, :] = sums[:, 0:128]
            ret_buf[s, 2 + i, :, :] = sums[:, 128:256]
        for k in range(4):
            ret_copy(s, k).start()

        @pl.when(s == 0)
        def _():
            for k in range(4):
                row = sidx[pl.ds(k, 1), :]
                hot_rows(pick_t, k, 0, 512, jnp.where(row < 0, -1, row & 511))

            def build_owned(c, carry):
                hot_rows(hot_t, c, 0, 512, split(rcv[pl.ds(c, 1), :])[0])
                return carry

            lax.fori_loop(0, edges // 128, build_owned, 0)

        for i in range(4):
            owned = scatter(i * 128, (i + 1) * 128)
            own_buf[s, i * 128 : (i + 1) * 128, :] = owned[:, 0:128]
            own_buf[s, 512 + i * 128 : 512 + (i + 1) * 128, :] = owned[:, 128:256]
        own_copy(s).start()

        for j in range(tiles):
            rows = pl.ds(j * tile, tile)
            message = msg2[0, rows, :].astype(F32) + msg2[1, rows, :].astype(F32)
            e[rows, :] = (e[rows, :].astype(F32) + message).astype(BF16)

        high = pick_hi[...] > 0
        places = beside(*[pick_t[k, :, :] for k in range(4)])

        def returned_sum(source):
            block = below(*[ret[s, source, k, :, :] for k in range(4)]).astype(F32)
            both = beside(jnp.where(high, 0.0, block), jnp.where(high, block, 0.0))
            return mm(places, both.astype(BF16))

        for k in range(4):
            ret_copy(s, k).wait_recv()
            relay_copy(s, k).start()
        own_copy(s).wait_recv()
        back_sum[...] = returned_sum(t)
        for h in range(2):
            rows = pl.ds(h * 512, 512)
            own_sum[rows, :] = own_buf[s, rows, :].astype(F32) + own_peer[s, rows, :].astype(F32)
            own_lin[rows, :] = mm_t(x[rows, :], n_in_t[s, :, 0:128])
        for k in range(4):
            relay_copy(s, k).wait_recv()

        back = back_sum[...] + returned_sum(1 - t)
        for h in range(2):
            rows = pl.ds(h * 512, 512)
            total = (own_sum[rows, :] + back[:, h * 128 : (h + 1) * 128]).astype(BF16)
            lin = own_lin[rows, :] + mm_t(total, n_in_t[s, :, 128:256])
            hidden = jnp.maximum(lin, 0.0).astype(BF16)
            update = layer_norm(mm(hidden, n_out_full[s, :, :]))
            x[rows, :] = (x[rows, :].astype(F32) + update).astype(BF16)

        @pl.when(s < LAYERS - 1)
        def _():
            fill_fwd(s + 1)
            for k in range(4):
                fwd_copy(s + 1, k).start()

        return carry

    lax.fori_loop(0, LAYERS, layer_step, 0)

    for s in range(LAYERS):
        for k in range(4):
            fwd_copy(s, k).wait_send()
            ret_copy(s, k).wait_send()
            relay_copy(s, k).wait_send()
        own_copy(s).wait_send()


def local(
    doms,
    node_latent, edge_latent, edge_sender, edge_receiver, edge_count, send_index,
    edge_in, edge_out, node_in, node_out,
):
    edges = edge_latent.shape[0]
    tile = min(512, edges)
    tiles = edges // tile
    vmem = pl.BlockSpec(memory_space=pltpu.VMEM)
    hbm = pl.BlockSpec(memory_space=pltpu.HBM)
    dma = pltpu.SemaphoreType.DMA
    scratch = [
        pltpu.VMEM((6, edges, 128), BF16),
        pltpu.VMEM((6, edges, 128), BF16),
        pltpu.VMEM((edges // 128, 768, 128), BF16),
        pltpu.VMEM((edges, 128), I32),
        pltpu.VMEM((edges, 128), F32),
        pltpu.VMEM((2, edges, 128), BF16),
        pltpu.VMEM((4, 512, 128), BF16),
        pltpu.VMEM((4, 512, 128), BF16),
        pltpu.VMEM((512, 128), I32),
        pltpu.VMEM((2, 768, 128), BF16),
        pltpu.VMEM((2, 768, 128), BF16),
        pltpu.VMEM((512, 256), F32),
        pltpu.VMEM((1024, 128), F32),
        pltpu.VMEM((1024, 128), F32),
        pltpu.VMEM((LAYERS, 128, 384), BF16),
        pltpu.VMEM((LAYERS, 128, 256), BF16),
        pltpu.VMEM((LAYERS, 128, 128), BF16),
        pltpu.VMEM((LAYERS, 128, 128), BF16),
        pltpu.VMEM((LAYERS, 256, 128), BF16),
        pltpu.VMEM((LAYERS, 2, 256, 128), BF16),
        pltpu.VMEM((LAYERS, 2, 256, 128), BF16),
        pltpu.VMEM((LAYERS, 4, 128, 128), BF16),
        pltpu.VMEM((LAYERS, 4, 128, 128), BF16),
        pltpu.VMEM((LAYERS, 4, 128, 128), BF16),
        pltpu.VMEM((LAYERS, 2, 4, 128, 128), BF16),
        pltpu.VMEM((LAYERS, 1024, 128), BF16),
        pltpu.VMEM((LAYERS, 1024, 128), BF16),
        dma, dma((4,)), dma((4,)),
        dma((LAYERS, 4)), dma((LAYERS, 4)), dma((LAYERS, 4)), dma((LAYERS, 4)),
        dma((LAYERS, 4)), dma((LAYERS, 4)), dma((LAYERS,)), dma((LAYERS,)),
    ]
    return pl.pallas_call(
        functools.partial(kernel, doms, tile),
        out_shape=(
            pltpu.VMEM(node_latent.shape, BF16),
            pltpu.VMEM(edge_latent.shape, BF16),
        ),
        in_specs=[vmem, hbm, vmem, vmem, pl.BlockSpec(memory_space=pltpu.SMEM)]
        + [vmem] * 5,
        out_specs=(vmem, vmem),
        scratch_shapes=scratch,
        compiler_params=pltpu.CompilerParams(
            collective_id=0, has_side_effects=True, vmem_limit_bytes=65700000,
        ),
    )(
        node_latent, edge_latent,
        edge_sender.reshape(-1, 128), edge_receiver.reshape(-1, 128),
        edge_count.reshape(1, 1), send_index.reshape(4, 128),
        jnp.swapaxes(edge_in, 1, 2), edge_out, jnp.swapaxes(node_in, 1, 2), node_out,
    )


def solution(mesh):
    return jax.shard_map(
        functools.partial(local, mesh.shape["dom"]),
        mesh=mesh,
        in_specs=(
            P("dom", None),
            P(("dom", "tp"), None),
            P(("dom", "tp")),
            P(("dom", "tp")),
            P(("dom", "tp")),
            P("dom", None, None),
            P(None, None, "tp"),
            P(None, "tp", None),
            P(None, None, "tp"),
            P(None, "tp", None),
        ),
        out_specs=(P("dom", None), P(("dom", "tp"), None)),
        check_vma=False,
    )
```

```python
import functools

import jax
import jax.numpy as jnp
from jax import lax
from jax.experimental import pallas as pl
from jax.experimental.pallas import tpu as pltpu
from jax.sharding import PartitionSpec as P

LAYERS = 3
OFFSETS = (1, -1, 2, -2)
NORM_FLOOR = 0.25
MESH = pl.DeviceIdType.MESH
F32 = jnp.float32
BF16 = jnp.bfloat16
I16 = jnp.int16
I32 = jnp.int32


def mm(a, b):
    return jnp.dot(a, b, preferred_element_type=F32)


def mm_t(a, b):
    return lax.dot_general(a, b, (((1,), (1,)), ((), ())), preferred_element_type=F32)


def beside(*parts):
    return jnp.concatenate(parts, axis=1)


def below(*parts):
    return jnp.concatenate(parts, axis=0)


def layer_norm(values):
    centre = jnp.mean(values, axis=-1, keepdims=True)
    centred = values - centre
    spread = jnp.mean(centred * centred, axis=-1, keepdims=True)
    return centred * lax.rsqrt(spread + NORM_FLOOR)


def hot(match):
    return jnp.where(match, jnp.ones((), BF16), jnp.zeros((), BF16))


def column(row):
    return jnp.transpose(jnp.broadcast_to(row, (128, 128)))


def pick_half(both, high):
    return jnp.where(high, both[:, 128:], both[:, :128])


def kernel(
    doms, tile,
    x_hbm, e_hbm, snd_hbm, rcv_hbm, cnt_hbm, sidx_hbm, w_in_hbm, w_out_hbm, n_in_hbm, n_out_hbm,
    x, e,
    snd, rcv, cnt, sidx, w_in, w_out, n_in, n_out,
    hot_s, hot_r, hot_t, code, acc, msg2,
    pick, pick_t, pick_hi, tab_s, tab_r, back_sum, own_sum, own_lin,
    w_in_t, n_in_t, w_out_full, n_out_full, w_sr_t, w_e2, w_o2,
    fwd_buf, halo, ret_buf, ret, own_buf, own_peer,
    in_sem, w_send, w_recv, fwd_send, fwd_recv, ret_send, ret_recv,
    rel_send, rel_recv, own_send, own_recv,
):
    p = lax.axis_index("dom")
    t = lax.axis_index("tp")
    peer = (p, 1 - t)
    to = [(lax.rem(p + o + doms, doms), 1 - t) for o in OFFSETS]
    back = [(lax.rem(p - o + doms, doms), 1 - t) for o in OFFSETS]
    edges = e.shape[0]
    tiles = edges // tile
    half = tile // 2
    chunks = tile // 128

    barrier = pltpu.get_barrier_semaphore()
    for other in to + [peer]:
        pl.semaphore_signal(barrier, inc=1, device_id=other, device_id_type=MESH)

    loads = [
        pltpu.make_async_copy(src, dst, in_sem.at[i])
        for i, (src, dst) in enumerate([
            (sidx_hbm, sidx), (x_hbm, x), (w_in_hbm, w_in), (w_out_hbm, w_out),
            (n_in_hbm, n_in), (n_out_hbm, n_out), (snd_hbm, snd), (rcv_hbm, rcv),
            (cnt_hbm, cnt), (e_hbm, e)])
    ]
    for copy in loads:
        copy.start()

    def remote(src, dst, send, recv, device):
        return pltpu.make_async_remote_copy(
            src_ref=src, dst_ref=dst, send_sem=send, recv_sem=recv,
            device_id=device, device_id_type=MESH,
        )

    def fwd_copy(layer, k):
        return remote(fwd_buf.at[layer, k], halo.at[layer, k],
                      fwd_send.at[layer, k], fwd_recv.at[layer, k], to[k])

    def ret_copy(layer, k):
        return remote(ret_buf.at[layer, k], ret.at[layer, 1 - t, k],
                      ret_send.at[layer, k], ret_recv.at[layer, k], back[k])

    def relay_copy(layer, k):
        return remote(ret.at[layer, t, k], ret.at[layer, t, k],
                      rel_send.at[layer, k], rel_recv.at[layer, k], peer)

    def own_copy(layer):
        return remote(own_buf.at[layer], own_peer.at[layer],
                      own_send.at[layer], own_recv.at[layer], peer)

    rows64 = pl.ds(pl.multiple_of(t * 64, 64), 64)
    weight_copies = [
        remote(src, dst.at[:, rows64, :], w_send.at[i], w_recv.at[i], peer)
        for i, (src, dst) in enumerate(
            [(w_in, w_in_t), (w_out, w_out_full), (n_in, n_in_t), (n_out, n_out_full)])
    ]

    lane = lax.broadcasted_iota(I32, (128, 128), 1)
    sub = lax.broadcasted_iota(I32, (128, 128), 0)
    sub16 = lax.broadcasted_iota(I32, (16, 128), 0).astype(I16)
    lane_of = [lax.broadcasted_iota(I32, (16, 128), 1) + g * 128 for g in range(6)]

    def hot_columns(ref, groups, start, low):
        for i in range(8):
            part = low[i * 16 : (i + 1) * 16, :]
            for g in range(groups):
                ref[g, pl.ds(start + i * 16, 16), :] = jnp.where(
                    part == lane_of[g], 1.0, 0.0).astype(BF16)

    def hot_rows(ref, c, row_from, row_to, low_row):
        wide = jnp.broadcast_to(low_row, (16, 128)).astype(I16)
        for i in range(row_from // 16, row_to // 16):
            ref[c, i * 16 : (i + 1) * 16, :] = hot(wide - I16(i * 16) == sub16)

    loads[0].wait()
    for k in range(4):
        row = sidx[pl.ds(k, 1), :]
        wide = column(row)
        rows = pl.ds(k * 128, 128)
        low = jnp.where(wide < 0, -1, wide & 511)
        pick_hi[rows, :] = jnp.where(wide >= 512, 1, 0)
        hot_columns(pick, 4, k * 128, low)

    def fill_fwd(layer):
        table = beside(x[0:512, :], x[512:1024, :])
        for h in range(4):
            rows = pl.ds(h * 128, 128)
            both = mm(beside(*[pick[g, rows, :] for g in range(4)]), table)
            fwd_buf[layer, h, :, :] = pick_half(both, pick_hi[rows, :] > 0).astype(BF16)

    loads[1].wait()
    fill_fwd(0)
    for copy in loads[2:6]:
        copy.wait()
    for src, dst in [(w_in, w_in_t), (w_out, w_out_full), (n_in, n_in_t), (n_out, n_out_full)]:
        dst[:, rows64, :] = src[...]
    w_e2[...] = jnp.zeros_like(w_e2)
    w_o2[...] = jnp.zeros_like(w_o2)
    pl.semaphore_wait(barrier, 5)
    for k in range(4):
        fwd_copy(0, k).start()
    for copy in weight_copies:
        copy.start()

    for copy in loads[6:]:
        copy.wait()
    live = cnt[0, 0]

    def split(row):
        own = row < 1024
        low = jnp.where(own, row & 511, 512 + (row & 255))
        high = jnp.where(own, row >> 9, (row >> 8) & 1)
        return low, high

    def build_one(c):
        start = c * 128
        rows = pl.ds(start, 128)
        low, high = split(snd[pl.ds(c, 1), :])
        low_r, high_r = split(rcv[pl.ds(c, 1), :])
        hot_rows(hot_t, c, 512, 768, low_r)
        both = column(low + high * 1024)
        both_r = column(low_r + high_r * 1024)
        hot_columns(hot_s, 6, start, both & 1023)
        hot_columns(hot_r, 6, start, both_r & 1023)
        alive = sub + start < live
        held = jnp.where(both_r >= 1024, jnp.where(alive, 6, 4), jnp.where(alive, 0, 2))
        code[rows, :] = held + (both >> 10)

    def build_tile(j):
        for c in range(chunks):
            build_one(j * chunks + c)

    def lay_out_weights(s):
        full = jnp.transpose(w_in_t[s, :, 0:128].astype(F32)).astype(BF16)
        w_e2[s, 0, 0:128, :] = full
        w_e2[s, 1, 128:256, :] = full
        w_sr_t[s, 0:128, :] = w_in_t[s, :, 128:256]
        w_sr_t[s, 128:256, :] = w_in_t[s, :, 256:384]
        full = w_out_full[s, :, :]
        w_o2[s, 0, 0:128, :] = full
        w_o2[s, 1, 128:256, :] = full

    def project_owned(s):
        for h in range(2):
            proj = mm_t(x[h * 512 : (h + 1) * 512, :], w_sr_t[s, :, :]).astype(BF16)
            tab_s[h, 0:512, :] = proj[:, 0:128]
            tab_r[h, 0:512, :] = proj[:, 128:256]

    def gather(hots, tab, rows, groups, table_rows):
        return mm(beside(*[hots[g, rows, :] for g in groups]),
                  beside(tab[0, table_rows, :], tab[1, table_rows, :]))

    def with_picked(lin, from_s, from_r, rows):
        held = code[rows, :]
        lin = lin + pick_half(from_s, (held & 1) > 0)
        return lin + pick_half(from_r, held >= 4)

    def owned_part(s, j):
        rows = pl.ds(j * tile, tile)
        owned_rows = pl.ds(0, 512)
        pair = beside(e[pl.ds(j * tile, half), :], e[pl.ds(j * tile + half, half), :])
        lin = mm(pair, beside(w_e2[s, 0, :, :], w_e2[s, 1, :, :]))
        lin = below(lin[:, 0:128], lin[:, 128:256])
        from_s = gather(hot_s, tab_s, rows, range(4), owned_rows)
        from_r = gather(hot_r, tab_r, rows, range(4), owned_rows)
        acc[rows, :] = with_picked(lin, from_s, from_r, rows)

    build_tile(0)
    build_tile(1)
    for copy in weight_copies:
        copy.wait()
    lay_out_weights(0)
    project_owned(0)
    for j in range(tiles):
        if j + 2 < tiles:
            build_tile(j + 2)
        owned_part(0, j)

    def layer_step(s, carry):
        for k in range(4):
            fwd_copy(s, k).wait_recv()
        for h in range(2):
            held = below(halo[s, 2 * h, :, :], halo[s, 2 * h + 1, :, :])
            proj = mm_t(held, w_sr_t[s, :, :]).astype(BF16)
            tab_s[h, 512:768, :] = proj[:, 0:128]
            tab_r[h, 512:768, :] = proj[:, 128:256]

        halo_rows = pl.ds(512, 256)

        def hidden_of(j):
            rows = pl.ds(j * tile, tile)
            from_s = gather(hot_s, tab_s, rows, (4, 5), halo_rows)
            from_r = gather(hot_r, tab_r, rows, (4, 5), halo_rows)
            lin = with_picked(acc[rows, :], from_s, from_r, rows)
            return jnp.maximum(lin, 0.0).astype(BF16)

        def message_of(j, hidden):
            rows = pl.ds(j * tile, tile)
            pair = beside(hidden[0:half, :], hidden[half:tile, :])
            out = mm(pair, beside(w_o2[s, 0, :, :], w_o2[s, 1, :, :]))
            out = layer_norm(below(out[:, 0:128], out[:, 128:256]))
            held = code[rows, :]
            msg2[0, rows, :] = jnp.where(held < 2, out, 0.0).astype(BF16)
            msg2[1, rows, :] = jnp.where(held >= 6, out, 0.0).astype(BF16)

        hidden = hidden_of(0)
        for j in range(tiles):
            later = hidden_of(j + 1) if j + 1 < tiles else None
            message_of(j, hidden)
            hidden = later

        def scatter(row_from, row_to):
            return mm(beside(*[hot_t[c, row_from:row_to, :] for c in range(edges // 128)]),
                      beside(msg2[0, 0:edges, :], msg2[1, 0:edges, :])).astype(BF16)

        for i in range(2):
            sums = scatter(512 + i * 128, 640 + i * 128)
            ret_buf[s, i, :, :] = sums[:, 0:128]
            ret_buf[s, 2 + i, :, :] = sums[:, 128:256]
        for k in range(4):
            ret_copy(s, k).start()

        @pl.when(s == 0)
        def _():
            for k in range(4):
                row = sidx[pl.ds(k, 1), :]
                hot_rows(pick_t, k, 0, 512, jnp.where(row < 0, -1, row & 511))

            def build_owned(c, carry):
                hot_rows(hot_t, c, 0, 512, split(rcv[pl.ds(c, 1), :])[0])
                return carry

            lax.fori_loop(0, edges // 128, build_owned, 0)
            for layer in range(1, LAYERS):
                lay_out_weights(layer)

        for i in range(4):
            owned = scatter(i * 128, (i + 1) * 128)
            own_buf[s, i * 128 : (i + 1) * 128, :] = owned[:, 0:128]
            own_buf[s, 512 + i * 128 : 512 + (i + 1) * 128, :] = owned[:, 128:256]
        own_copy(s).start()

        for j in range(tiles):
            rows = pl.ds(j * tile, tile)
            message = msg2[0, rows, :].astype(F32) + msg2[1, rows, :].astype(F32)
            e[rows, :] = (e[rows, :].astype(F32) + message).astype(BF16)

        for k in range(4):
            fwd_copy(s, k).wait_send()

        high = pick_hi[...] > 0
        places = beside(*[pick_t[k, :, :] for k in range(4)])

        def returned_sum(source):
            block = below(*[ret[s, source, k, :, :] for k in range(4)]).astype(F32)
            both = beside(jnp.where(high, 0.0, block), jnp.where(high, block, 0.0))
            both = both.astype(BF16)
            return below(mm(places[0:256, :], both), mm(places[256:512, :], both))

        for k in range(4):
            ret_copy(s, k).wait_recv()
            relay_copy(s, k).start()
        own_copy(s).wait_recv()
        for k in range(4):
            ret_copy(s, k).wait_send()
        own_copy(s).wait_send()
        back_sum[...] = returned_sum(t)
        for h in range(2):
            rows = pl.ds(h * 512, 512)
            own_sum[rows, :] = own_buf[s, rows, :].astype(F32) + own_peer[s, rows, :].astype(F32)
            own_lin[rows, :] = mm_t(x[rows, :], n_in_t[s, :, 0:128])
        for k in range(4):
            relay_copy(s, k).wait_recv()

        back = back_sum[...] + returned_sum(1 - t)
        for h in range(2):
            rows = pl.ds(h * 512, 512)
            total = (own_sum[rows, :] + back[:, h * 128 : (h + 1) * 128]).astype(BF16)
            lin = own_lin[rows, :] + mm_t(total, n_in_t[s, :, 128:256])
            hidden = jnp.maximum(lin, 0.0).astype(BF16)
            update = layer_norm(mm(hidden, n_out_full[s, :, :]))
            x[rows, :] = (x[rows, :].astype(F32) + update).astype(BF16)

        @pl.when(s < LAYERS - 1)
        def _():
            fill_fwd(s + 1)
            for k in range(4):
                fwd_copy(s + 1, k).start()

        @pl.when(s < LAYERS - 1)
        def _():
            project_owned(s + 1)
            for j in range(tiles):
                owned_part(s + 1, j)

        for k in range(4):
            relay_copy(s, k).wait_send()
        return carry

    lax.fori_loop(0, LAYERS, layer_step, 0)


def local(
    doms,
    node_latent, edge_latent, edge_sender, edge_receiver, edge_count, send_index,
    edge_in, edge_out, node_in, node_out,
):
    edges = edge_latent.shape[0]
    tile = min(512, edges)
    tiles = edges // tile
    vmem = pl.BlockSpec(memory_space=pltpu.VMEM)
    hbm = pl.BlockSpec(memory_space=pltpu.HBM)
    dma = pltpu.SemaphoreType.DMA
    packed = (edges // 128, 128)
    scratch = [
        pltpu.VMEM(packed, I32),
        pltpu.VMEM(packed, I32),
        pltpu.SMEM((1, 1), I32),
        pltpu.VMEM((4, 128), I32),
        pltpu.VMEM((LAYERS, 64, 384), BF16),
        pltpu.VMEM((LAYERS, 64, 128), BF16),
        pltpu.VMEM((LAYERS, 64, 256), BF16),
        pltpu.VMEM((LAYERS, 64, 128), BF16),
        pltpu.VMEM((6, edges, 128), BF16),
        pltpu.VMEM((6, edges, 128), BF16),
        pltpu.VMEM((edges // 128, 768, 128), BF16),
        pltpu.VMEM((edges, 128), I32),
        pltpu.VMEM((edges, 128), F32),
        pltpu.VMEM((2, edges, 128), BF16),
        pltpu.VMEM((4, 512, 128), BF16),
        pltpu.VMEM((4, 512, 128), BF16),
        pltpu.VMEM((512, 128), I32),
        pltpu.VMEM((2, 768, 128), BF16),
        pltpu.VMEM((2, 768, 128), BF16),
        pltpu.VMEM((512, 256), F32),
        pltpu.VMEM((1024, 128), F32),
        pltpu.VMEM((1024, 128), F32),
        pltpu.VMEM((LAYERS, 128, 384), BF16),
        pltpu.VMEM((LAYERS, 128, 256), BF16),
        pltpu.VMEM((LAYERS, 128, 128), BF16),
        pltpu.VMEM((LAYERS, 128, 128), BF16),
        pltpu.VMEM((LAYERS, 256, 128), BF16),
        pltpu.VMEM((LAYERS, 2, 256, 128), BF16),
        pltpu.VMEM((LAYERS, 2, 256, 128), BF16),
        pltpu.VMEM((LAYERS, 4, 128, 128), BF16),
        pltpu.VMEM((LAYERS, 4, 128, 128), BF16),
        pltpu.VMEM((LAYERS, 4, 128, 128), BF16),
        pltpu.VMEM((LAYERS, 2, 4, 128, 128), BF16),
        pltpu.VMEM((LAYERS, 1024, 128), BF16),
        pltpu.VMEM((LAYERS, 1024, 128), BF16),
        dma((10,)), dma((4,)), dma((4,)),
        dma((LAYERS, 4)), dma((LAYERS, 4)), dma((LAYERS, 4)), dma((LAYERS, 4)),
        dma((LAYERS, 4)), dma((LAYERS, 4)), dma((LAYERS,)), dma((LAYERS,)),
    ]
    return pl.pallas_call(
        functools.partial(kernel, doms, tile),
        out_shape=(
            pltpu.VMEM(node_latent.shape, BF16),
            pltpu.VMEM(edge_latent.shape, BF16),
        ),
        in_specs=[hbm] * 10,
        out_specs=(vmem, vmem),
        scratch_shapes=scratch,
        compiler_params=pltpu.CompilerParams(
            collective_id=0, has_side_effects=True, vmem_limit_bytes=65700000,
        ),
    )(
        node_latent, edge_latent,
        edge_sender.reshape(-1, 128), edge_receiver.reshape(-1, 128),
        edge_count.reshape(1, 1), send_index.reshape(4, 128),
        jnp.swapaxes(edge_in, 1, 2), edge_out, jnp.swapaxes(node_in, 1, 2), node_out,
    )


def solution(mesh):
    return jax.shard_map(
        functools.partial(local, mesh.shape["dom"]),
        mesh=mesh,
        in_specs=(
            P("dom", None),
            P(("dom", "tp"), None),
            P(("dom", "tp")),
            P(("dom", "tp")),
            P(("dom", "tp")),
            P("dom", None, None),
            P(None, None, "tp"),
            P(None, "tp", None),
            P(None, None, "tp"),
            P(None, "tp", None),
        ),
        out_specs=(P("dom", None), P(("dom", "tp"), None)),
        check_vma=False,
    )
```

```python
import functools

import jax
import jax.numpy as jnp
from jax import lax
from jax.experimental import pallas as pl
from jax.experimental.pallas import tpu as pltpu
from jax.sharding import PartitionSpec as P

LAYERS = 3
OFFSETS = (1, -1, 2, -2)
NORM_FLOOR = 0.25
MESH = pl.DeviceIdType.MESH
F32 = jnp.float32
BF16 = jnp.bfloat16
I16 = jnp.int16
I32 = jnp.int32


def mm(a, b):
    return jnp.dot(a, b, preferred_element_type=F32)


def mm_t(a, b):
    return lax.dot_general(a, b, (((1,), (1,)), ((), ())), preferred_element_type=F32)


def beside(*parts):
    return jnp.concatenate(parts, axis=1)


def below(*parts):
    return jnp.concatenate(parts, axis=0)


def norm_centred(values):
    spread = jnp.sum(values * values, axis=-1, keepdims=True) * (1.0 / 128.0)
    return values * lax.rsqrt(spread + NORM_FLOOR)


def centred(weights):
    wide = weights.astype(F32)
    return (wide - jnp.mean(wide, axis=-1, keepdims=True)).astype(BF16)


def hot(match):
    return jnp.where(match, jnp.ones((), BF16), jnp.zeros((), BF16))


def column(row):
    return jnp.transpose(jnp.broadcast_to(row, (128, 128)))


def pick_half(both, high):
    return jnp.where(high, both[:, 128:], both[:, :128])


def kernel(
    doms, tile,
    x_hbm, e_hbm, snd_hbm, rcv_hbm, cnt_hbm, sidx_hbm, w_in_hbm, w_out_hbm, n_in_hbm, n_out_hbm,
    x, e,
    snd, rcv, cnt, sidx, w_in, w_out, n_in, n_out,
    hot_s, hot_r, hot_t, code, acc, msg2,
    pick, pick_t, pick_hi, tab_s, tab_r, back_sum, own_sum, own_lin,
    w_in_t, n_in_t, w_out_full, n_out_full, n_out_mid, w_sr_t, w_e2, w_o2,
    fwd_buf, halo, ret_buf, ret, own_buf, own_peer,
    in_sem, send_sem, w_recv, fwd_recv, ret_recv, rel_recv, own_recv,
):
    p = lax.axis_index("dom")
    t = lax.axis_index("tp")
    peer = (p, 1 - t)
    to = [(lax.rem(p + o + doms, doms), 1 - t) for o in OFFSETS]
    back = [(lax.rem(p - o + doms, doms), 1 - t) for o in OFFSETS]
    edges = e.shape[0]
    tiles = edges // tile
    half = tile // 2
    chunks = tile // 128

    barrier = pltpu.get_barrier_semaphore()
    for other in to + [peer]:
        pl.semaphore_signal(barrier, inc=1, device_id=other, device_id_type=MESH)

    loads = [
        pltpu.make_async_copy(src, dst, in_sem.at[i])
        for i, (src, dst) in enumerate([
            (sidx_hbm, sidx), (x_hbm, x), (w_in_hbm, w_in), (w_out_hbm, w_out),
            (n_in_hbm, n_in), (n_out_hbm, n_out), (snd_hbm, snd), (rcv_hbm, rcv),
            (cnt_hbm, cnt), (e_hbm, e)])
    ]
    for copy in loads:
        copy.start()

    def remote(src, dst, send, recv, device):
        return pltpu.make_async_remote_copy(
            src_ref=src, dst_ref=dst, send_sem=send, recv_sem=recv,
            device_id=device, device_id_type=MESH,
        )

    def fwd_copy(layer, *k):
        return remote(fwd_buf.at[(layer, *k)], halo.at[(layer, *k)],
                      send_sem.at[0], fwd_recv.at[layer], to[k[0] if k else 0])

    def ret_copy(layer, *k):
        return remote(ret_buf.at[(layer, *k)], ret.at[(layer, 1 - t, *k)],
                      send_sem.at[1], ret_recv.at[layer, k[0] if k else 0], back[k[0] if k else 0])

    def relay_copy(layer, *k):
        return remote(ret.at[(layer, t, *k)], ret.at[(layer, t, *k)],
                      send_sem.at[2], rel_recv.at[layer], peer)

    def own_copy(layer):
        return remote(own_buf.at[layer], own_peer.at[layer],
                      send_sem.at[3], own_recv.at[layer], peer)

    rows64 = pl.ds(pl.multiple_of(t * 64, 64), 64)
    weight_copies = [
        remote(src, dst.at[:, rows64, :], in_sem.at[2 + i], w_recv.at[i], peer)
        for i, (src, dst) in enumerate(
            [(w_in, w_in_t), (w_out, w_out_full), (n_in, n_in_t), (n_out, n_out_full)])
    ]

    lane = lax.broadcasted_iota(I32, (128, 128), 1)
    sub = lax.broadcasted_iota(I32, (128, 128), 0)
    sub16 = lax.broadcasted_iota(I32, (16, 128), 0).astype(I16)
    lane_of = [lax.broadcasted_iota(I32, (16, 128), 1) + g * 128 for g in range(6)]

    def hot_columns(ref, groups, start, low):
        for i in range(8):
            part = low[i * 16 : (i + 1) * 16, :]
            for g in range(groups):
                ref[g, pl.ds(start + i * 16, 16), :] = jnp.where(
                    part == lane_of[g], 1.0, 0.0).astype(BF16)

    def hot_rows(ref, c, row_from, row_to, low_row):
        wide = jnp.broadcast_to(low_row, (16, 128)).astype(I16)
        for i in range(row_from // 16, row_to // 16):
            ref[c, i * 16 : (i + 1) * 16, :] = hot(wide - I16(i * 16) == sub16)

    loads[0].wait()
    for k in range(4):
        row = sidx[pl.ds(k, 1), :]
        wide = column(row)
        rows = pl.ds(k * 128, 128)
        low = jnp.where(wide < 0, -1, wide & 511)
        pick_hi[rows, :] = jnp.where(wide >= 512, 1, 0)
        hot_columns(pick, 4, k * 128, low)

    def fill_fwd(layer):
        table = beside(x[0:512, :], x[512:1024, :])
        for h in range(4):
            rows = pl.ds(h * 128, 128)
            both = mm(beside(*[pick[g, rows, :] for g in range(4)]), table)
            fwd_buf[layer, h, :, :] = pick_half(both, pick_hi[rows, :] > 0).astype(BF16)

    loads[1].wait()
    fill_fwd(0)
    for copy in loads[2:6]:
        copy.wait()
    for src, dst in [(w_in, w_in_t), (w_out, w_out_full), (n_in, n_in_t), (n_out, n_out_full)]:
        dst[:, rows64, :] = src[...]
    w_e2[...] = jnp.zeros_like(w_e2)
    w_o2[...] = jnp.zeros_like(w_o2)
    pl.semaphore_wait(barrier, 5)
    for k in range(4):
        fwd_copy(0, k).start()
    for copy in weight_copies:
        copy.start()

    for copy in loads[6:]:
        copy.wait()
    live = cnt[0, 0]

    def split(row):
        own = row < 1024
        low = jnp.where(own, row & 511, 512 + (row & 255))
        high = jnp.where(own, row >> 9, (row >> 8) & 1)
        return low, high

    def build_one(c):
        start = c * 128
        rows = pl.ds(start, 128)
        low, high = split(snd[pl.ds(c, 1), :])
        low_r, high_r = split(rcv[pl.ds(c, 1), :])
        hot_rows(hot_t, c, 512, 768, low_r)
        both = column(low + high * 1024)
        both_r = column(low_r + high_r * 1024)
        hot_columns(hot_s, 6, start, both & 1023)
        hot_columns(hot_r, 6, start, both_r & 1023)
        alive = sub + start < live
        held = jnp.where(both_r >= 1024, jnp.where(alive, 6, 4), jnp.where(alive, 0, 2))
        code[rows, :] = held + (both >> 10)

    def build_tile(j):
        for c in range(chunks):
            build_one(j * chunks + c)

    def lay_out_weights(s):
        full = jnp.transpose(w_in_t[s, :, 0:128].astype(F32)).astype(BF16)
        w_e2[s, 0, 0:128, :] = full
        w_e2[s, 1, 128:256, :] = full
        w_sr_t[s, 0:128, :] = w_in_t[s, :, 128:256]
        w_sr_t[s, 128:256, :] = w_in_t[s, :, 256:384]
        full = centred(w_out_full[s, :, :])
        w_o2[s, 0, 0:128, :] = full
        w_o2[s, 1, 128:256, :] = full

    def project_owned(s):
        for h in range(2):
            proj = mm_t(x[h * 512 : (h + 1) * 512, :], w_sr_t[s, :, :]).astype(BF16)
            tab_s[h, 0:512, :] = proj[:, 0:128]
            tab_r[h, 0:512, :] = proj[:, 128:256]

    def gather(hots, tab, rows, groups, table_rows):
        return mm(beside(*[hots[g, rows, :] for g in groups]),
                  beside(tab[0, table_rows, :], tab[1, table_rows, :]))

    def with_picked(lin, from_s, from_r, rows):
        held = code[rows, :]
        lin = lin + pick_half(from_s, (held & 1) > 0)
        return lin + pick_half(from_r, held >= 4)

    def owned_part(s, j):
        rows = pl.ds(j * tile, tile)
        owned_rows = pl.ds(0, 512)
        pair = beside(e[pl.ds(j * tile, half), :], e[pl.ds(j * tile + half, half), :])
        lin = mm(pair, beside(w_e2[s, 0, :, :], w_e2[s, 1, :, :]))
        lin = below(lin[:, 0:128], lin[:, 128:256])
        from_s = gather(hot_s, tab_s, rows, range(4), owned_rows)
        from_r = gather(hot_r, tab_r, rows, range(4), owned_rows)
        acc[rows, :] = with_picked(lin, from_s, from_r, rows)

    build_tile(0)
    build_tile(1)
    for copy in weight_copies:
        copy.wait()
    lay_out_weights(0)
    project_owned(0)
    for j in range(tiles):
        if j + 2 < tiles:
            build_tile(j + 2)
        owned_part(0, j)

    def layer_step(s, carry):
        fwd_copy(s).wait_recv()
        for h in range(2):
            held = below(halo[s, 2 * h, :, :], halo[s, 2 * h + 1, :, :])
            proj = mm_t(held, w_sr_t[s, :, :]).astype(BF16)
            tab_s[h, 512:768, :] = proj[:, 0:128]
            tab_r[h, 512:768, :] = proj[:, 128:256]

        halo_rows = pl.ds(512, 256)

        def hidden_of(j):
            rows = pl.ds(j * tile, tile)
            from_s = gather(hot_s, tab_s, rows, (4, 5), halo_rows)
            from_r = gather(hot_r, tab_r, rows, (4, 5), halo_rows)
            lin = with_picked(acc[rows, :], from_s, from_r, rows)
            return jnp.maximum(lin, 0.0).astype(BF16)

        def message_of(j, hidden):
            rows = pl.ds(j * tile, tile)
            pair = beside(hidden[0:half, :], hidden[half:tile, :])
            out = mm(pair, beside(w_o2[s, 0, :, :], w_o2[s, 1, :, :]))
            out = norm_centred(below(out[:, 0:128], out[:, 128:256]))
            held = code[rows, :]
            msg2[0, rows, :] = jnp.where(held < 2, out, 0.0).astype(BF16)
            msg2[1, rows, :] = jnp.where(held >= 6, out, 0.0).astype(BF16)

        hidden = hidden_of(0)
        for j in range(tiles):
            later = hidden_of(j + 1) if j + 1 < tiles else None
            message_of(j, hidden)
            hidden = later

        def scatter(row_from, row_to):
            return mm(beside(*[hot_t[c, row_from:row_to, :] for c in range(edges // 128)]),
                      beside(msg2[0, 0:edges, :], msg2[1, 0:edges, :])).astype(BF16)

        for i in range(2):
            sums = scatter(512 + i * 128, 640 + i * 128)
            ret_buf[s, i, :, :] = sums[:, 0:128]
            ret_buf[s, 2 + i, :, :] = sums[:, 128:256]
        for k in range(4):
            ret_copy(s, k).start()

        @pl.when(s == 0)
        def _():
            for k in range(4):
                row = sidx[pl.ds(k, 1), :]
                hot_rows(pick_t, k, 0, 512, jnp.where(row < 0, -1, row & 511))

            def build_owned(c, carry):
                hot_rows(hot_t, c, 0, 512, split(rcv[pl.ds(c, 1), :])[0])
                return carry

            lax.fori_loop(0, edges // 128, build_owned, 0)
            for layer in range(LAYERS):
                n_out_mid[layer, :, :] = centred(n_out_full[layer, :, :])
                if layer > 0:
                    lay_out_weights(layer)

        for i in range(4):
            owned = scatter(i * 128, (i + 1) * 128)
            own_buf[s, i * 128 : (i + 1) * 128, :] = owned[:, 0:128]
            own_buf[s, 512 + i * 128 : 512 + (i + 1) * 128, :] = owned[:, 128:256]
        own_copy(s).start()

        for j in range(tiles):
            rows = pl.ds(j * tile, tile)
            message = msg2[0, rows, :].astype(F32) + msg2[1, rows, :].astype(F32)
            e[rows, :] = (e[rows, :].astype(F32) + message).astype(BF16)

        fwd_copy(s).wait_send()

        high = pick_hi[...] > 0
        places = beside(*[pick_t[k, :, :] for k in range(4)])

        def returned_sum(source):
            block = below(*[ret[s, source, k, :, :] for k in range(4)]).astype(F32)
            both = beside(jnp.where(high, 0.0, block), jnp.where(high, block, 0.0))
            both = both.astype(BF16)
            return below(mm(places[0:256, :], both), mm(places[256:512, :], both))

        for k in range(4):
            ret_copy(s, k).wait_recv()
            relay_copy(s, k).start()
        own_copy(s).wait_recv()
        ret_copy(s).wait_send()
        own_copy(s).wait_send()
        back_sum[...] = returned_sum(t)
        for h in range(2):
            rows = pl.ds(h * 512, 512)
            own_sum[rows, :] = own_buf[s, rows, :].astype(F32) + own_peer[s, rows, :].astype(F32)
            own_lin[rows, :] = mm_t(x[rows, :], n_in_t[s, :, 0:128])
        relay_copy(s).wait_recv()

        back = back_sum[...] + returned_sum(1 - t)
        for h in range(2):
            rows = pl.ds(h * 512, 512)
            total = (own_sum[rows, :] + back[:, h * 128 : (h + 1) * 128]).astype(BF16)
            lin = own_lin[rows, :] + mm_t(total, n_in_t[s, :, 128:256])
            hidden = jnp.maximum(lin, 0.0).astype(BF16)
            update = norm_centred(mm(hidden, n_out_mid[s, :, :]))
            x[rows, :] = (x[rows, :].astype(F32) + update).astype(BF16)

        @pl.when(s < LAYERS - 1)
        def _():
            fill_fwd(s + 1)
            for k in range(4):
                fwd_copy(s + 1, k).start()

        @pl.when(s < LAYERS - 1)
        def _():
            project_owned(s + 1)
            for j in range(tiles):
                owned_part(s + 1, j)

        relay_copy(s).wait_send()
        return carry

    lax.fori_loop(0, LAYERS, layer_step, 0)


def copy_out(x, e, x_out, e_out, sem):
    copies = [
        pltpu.make_async_copy(e, e_out, sem.at[0]),
        pltpu.make_async_copy(x, x_out, sem.at[1]),
    ]
    for copy in copies:
        copy.start()
    for copy in copies:
        copy.wait()


def local(
    doms,
    node_latent, edge_latent, edge_sender, edge_receiver, edge_count, send_index,
    edge_in, edge_out, node_in, node_out,
):
    edges = edge_latent.shape[0]
    tile = min(512, edges)
    tiles = edges // tile
    vmem = pl.BlockSpec(memory_space=pltpu.VMEM)
    hbm = pl.BlockSpec(memory_space=pltpu.HBM)
    dma = pltpu.SemaphoreType.DMA
    packed = (edges // 128, 128)
    scratch = [
        pltpu.VMEM(packed, I32),
        pltpu.VMEM(packed, I32),
        pltpu.SMEM((1, 1), I32),
        pltpu.VMEM((4, 128), I32),
        pltpu.VMEM((LAYERS, 64, 384), BF16),
        pltpu.VMEM((LAYERS, 64, 128), BF16),
        pltpu.VMEM((LAYERS, 64, 256), BF16),
        pltpu.VMEM((LAYERS, 64, 128), BF16),
        pltpu.VMEM((6, edges, 128), BF16),
        pltpu.VMEM((6, edges, 128), BF16),
        pltpu.VMEM((edges // 128, 768, 128), BF16),
        pltpu.VMEM((edges, 128), I32),
        pltpu.VMEM((edges, 128), F32),
        pltpu.VMEM((2, edges, 128), BF16),
        pltpu.VMEM((4, 512, 128), BF16),
        pltpu.VMEM((4, 512, 128), BF16),
        pltpu.VMEM((512, 128), I32),
        pltpu.VMEM((2, 768, 128), BF16),
        pltpu.VMEM((2, 768, 128), BF16),
        pltpu.VMEM((512, 256), F32),
        pltpu.VMEM((1024, 128), F32),
        pltpu.VMEM((1024, 128), F32),
        pltpu.VMEM((LAYERS, 128, 384), BF16),
        pltpu.VMEM((LAYERS, 128, 256), BF16),
        pltpu.VMEM((LAYERS, 128, 128), BF16),
        pltpu.VMEM((LAYERS, 128, 128), BF16),
        pltpu.VMEM((LAYERS, 128, 128), BF16),
        pltpu.VMEM((LAYERS, 256, 128), BF16),
        pltpu.VMEM((LAYERS, 2, 256, 128), BF16),
        pltpu.VMEM((LAYERS, 2, 256, 128), BF16),
        pltpu.VMEM((LAYERS, 4, 128, 128), BF16),
        pltpu.VMEM((LAYERS, 4, 128, 128), BF16),
        pltpu.VMEM((LAYERS, 4, 128, 128), BF16),
        pltpu.VMEM((LAYERS, 2, 4, 128, 128), BF16),
        pltpu.VMEM((LAYERS, 1024, 128), BF16),
        pltpu.VMEM((LAYERS, 1024, 128), BF16),
        dma((10,)), dma((4,)), dma((4,)), dma((LAYERS,)), dma((LAYERS, 4)),
        dma((LAYERS,)), dma((LAYERS,)),
    ]
    nodes, edges_now = pl.pallas_call(
        functools.partial(kernel, doms, tile),
        out_shape=(
            pltpu.VMEM(node_latent.shape, BF16),
            pltpu.VMEM(edge_latent.shape, BF16),
        ),
        in_specs=[hbm] * 10,
        out_specs=(vmem, vmem),
        scratch_shapes=scratch,
        compiler_params=pltpu.CompilerParams(
            collective_id=0, has_side_effects=True, vmem_limit_bytes=65700000,
        ),
    )(
        node_latent, edge_latent,
        edge_sender.reshape(-1, 128), edge_receiver.reshape(-1, 128),
        edge_count.reshape(1, 1), send_index.reshape(4, 128),
        jnp.swapaxes(edge_in, 1, 2), edge_out, jnp.swapaxes(node_in, 1, 2), node_out,
    )
    anywhere = pl.BlockSpec(memory_space=pl.ANY)
    return pl.pallas_call(
        copy_out,
        out_shape=(
            jax.ShapeDtypeStruct(node_latent.shape, BF16),
            jax.ShapeDtypeStruct(edge_latent.shape, BF16),
        ),
        in_specs=[anywhere, anywhere],
        out_specs=(anywhere, anywhere),
        scratch_shapes=[dma((2,))],
        compiler_params=pltpu.CompilerParams(vmem_limit_bytes=8 << 20),
    )(nodes, edges_now)


def solution(mesh):
    return jax.shard_map(
        functools.partial(local, mesh.shape["dom"]),
        mesh=mesh,
        in_specs=(
            P("dom", None),
            P(("dom", "tp"), None),
            P(("dom", "tp")),
            P(("dom", "tp")),
            P(("dom", "tp")),
            P("dom", None, None),
            P(None, None, "tp"),
            P(None, "tp", None),
            P(None, None, "tp"),
            P(None, "tp", None),
        ),
        out_specs=(P("dom", None), P(("dom", "tp"), None)),
        check_vma=False,
    )
```

```python
import functools

import jax
import jax.numpy as jnp
from jax import lax
from jax.experimental import pallas as pl
from jax.experimental.pallas import tpu as pltpu
from jax.sharding import PartitionSpec as P

LAYERS = 3
OFFSETS = (1, -1, 2, -2)
NORM_FLOOR = 0.25
MESH = pl.DeviceIdType.MESH
F32 = jnp.float32
BF16 = jnp.bfloat16
I16 = jnp.int16
I32 = jnp.int32


def mm(a, b):
    return jnp.dot(a, b, preferred_element_type=F32)


def mm_t(a, b):
    return lax.dot_general(a, b, (((1,), (1,)), ((), ())), preferred_element_type=F32)


def beside(*parts):
    return jnp.concatenate(parts, axis=1)


def below(*parts):
    return jnp.concatenate(parts, axis=0)


def norm_centred(values):
    spread = jnp.sum(values * values, axis=-1, keepdims=True) * (1.0 / 128.0)
    return values * lax.rsqrt(spread + NORM_FLOOR)


def centred(weights):
    wide = weights.astype(F32)
    return (wide - jnp.mean(wide, axis=-1, keepdims=True)).astype(BF16)


def hot(match):
    return jnp.where(match, jnp.ones((), BF16), jnp.zeros((), BF16))


def column(row):
    return jnp.transpose(jnp.broadcast_to(row, (128, 128)))


def pick_half(both, high):
    return jnp.where(high, both[:, 128:], both[:, :128])


def kernel(
    doms, tile,
    x_hbm, e_hbm, snd_hbm, rcv_hbm, cnt_hbm, sidx_hbm, w_in_hbm, w_out_hbm, n_in_hbm, n_out_hbm,
    x, e,
    snd, rcv, codes, cnt, sidx, w_in, w_out, n_in, n_out,
    hot_s, hot_r, hot_t, code, acc, msg2,
    pick, pick_t, pick_hi, tab_s, tab_r, back_sum, own_sum, own_lin,
    same, sent_x, sent_lin, sent_sum, sent_back,
    w_in_t, n_in_t, w_out_full, n_out_full, n_out_mid, w_sr_t, w_e2, w_o2,
    fwd_buf, halo, ret_buf, ret, own_buf, own_peer,
    in_sem, send_sem, w_recv, fwd_recv, ret_recv, rel_recv, own_recv,
):
    p = lax.axis_index("dom")
    t = lax.axis_index("tp")
    peer = (p, 1 - t)
    to = [(lax.rem(p + o + doms, doms), 1 - t) for o in OFFSETS]
    back = [(lax.rem(p - o + doms, doms), 1 - t) for o in OFFSETS]
    edges = e.shape[0]
    tiles = edges // tile
    half = tile // 2
    chunks = tile // 128

    barrier = pltpu.get_barrier_semaphore()
    for other in to + [peer]:
        pl.semaphore_signal(barrier, inc=1, device_id=other, device_id_type=MESH)

    loads = [
        pltpu.make_async_copy(src, dst, in_sem.at[i])
        for i, (src, dst) in enumerate([
            (sidx_hbm, sidx), (x_hbm, x), (w_in_hbm, w_in), (w_out_hbm, w_out),
            (n_in_hbm, n_in), (n_out_hbm, n_out), (snd_hbm, snd), (rcv_hbm, rcv),
            (cnt_hbm, cnt), (e_hbm, e)])
    ]
    for copy in loads:
        copy.start()

    def remote(src, dst, send, recv, device):
        return pltpu.make_async_remote_copy(
            src_ref=src, dst_ref=dst, send_sem=send, recv_sem=recv,
            device_id=device, device_id_type=MESH,
        )

    def fwd_copy(layer, *k):
        return remote(fwd_buf.at[(layer, *k)], halo.at[(layer, *k)],
                      send_sem.at[0], fwd_recv.at[layer], to[k[0] if k else 0])

    def ret_copy(layer, *k):
        return remote(ret_buf.at[(layer, *k)], ret.at[(layer, 1 - t, *k)],
                      send_sem.at[1], ret_recv.at[layer, k[0] if k else 0], back[k[0] if k else 0])

    def relay_copy(layer, *k):
        return remote(ret.at[(layer, t, *k)], ret.at[(layer, t, *k)],
                      send_sem.at[2], rel_recv.at[layer], peer)

    def own_copy(layer):
        return remote(own_buf.at[layer], own_peer.at[layer],
                      send_sem.at[3], own_recv.at[layer], peer)

    rows64 = pl.ds(pl.multiple_of(t * 64, 64), 64)
    weight_copies = [
        remote(src, dst.at[:, rows64, :], in_sem.at[2 + i], w_recv.at[i], peer)
        for i, (src, dst) in enumerate(
            [(w_in, w_in_t), (w_out, w_out_full), (n_in, n_in_t), (n_out, n_out_full)])
    ]

    lane = lax.broadcasted_iota(I32, (128, 128), 1)
    sub = lax.broadcasted_iota(I32, (128, 128), 0)
    sub16 = lax.broadcasted_iota(I32, (16, 128), 0).astype(I16)
    lane_of = [lax.broadcasted_iota(I32, (16, 128), 1) + g * 128 for g in range(6)]

    def hot_columns(ref, groups, start, low):
        for i in range(8):
            part = low[i * 16 : (i + 1) * 16, :]
            for g in range(groups):
                ref[g, pl.ds(start + i * 16, 16), :] = jnp.where(
                    part == lane_of[g], 1.0, 0.0).astype(BF16)

    def hot_rows(ref, c, row_from, row_to, low_row):
        wide = jnp.broadcast_to(low_row, (16, 128)).astype(I16)
        for i in range(row_from // 16, row_to // 16):
            ref[c, i * 16 : (i + 1) * 16, :] = hot(wide - I16(i * 16) == sub16)

    w_e2[...] = jnp.zeros_like(w_e2)
    w_o2[...] = jnp.zeros_like(w_o2)

    loads[0].wait()
    for k in range(4):
        row = sidx[pl.ds(k, 1), :]
        wide = column(row)
        rows = pl.ds(k * 128, 128)
        low = jnp.where(wide < 0, -1, wide & 511)
        pick_hi[rows, :] = jnp.where(wide >= 512, 1, 0)
        hot_columns(pick, 4, k * 128, low)

    def picked(top, bottom):
        table = beside(top, bottom)
        parts = []
        for h in range(2):
            rows = pl.ds(h * 256, 256)
            both = mm(beside(*[pick[g, rows, :] for g in range(4)]), table)
            parts.append(pick_half(both, pick_hi[rows, :] > 0))
        return below(*parts)

    def fill_fwd(layer, rows):
        for k in range(4):
            fwd_buf[layer, k, :, :] = rows[k * 128 : (k + 1) * 128, :]

    loads[1].wait()
    fill_fwd(0, picked(x[0:512, :], x[512:1024, :]).astype(BF16))
    for copy in loads[2:6]:
        copy.wait()
    for src, dst in [(w_in, w_in_t), (w_out, w_out_full), (n_in, n_in_t), (n_out, n_out_full)]:
        dst[:, rows64, :] = src[...]
    pl.semaphore_wait(barrier, 5)
    for k in range(4):
        fwd_copy(0, k).start()
    for copy in weight_copies:
        copy.start()

    for copy in loads[6:]:
        copy.wait()
    live = cnt[0, 0]

    def split(row):
        own = row < 1024
        low = jnp.where(own, row & 511, 512 + (row & 255))
        high = jnp.where(own, row >> 9, (row >> 8) & 1)
        return low, high

    low, high_s = split(snd[...])
    snd[...] = low
    low, high = split(rcv[...])
    rcv[...] = low
    slot = (lax.broadcasted_iota(I32, snd.shape, 0) * 128
            + lax.broadcasted_iota(I32, snd.shape, 1))
    alive = slot < live
    codes[...] = high_s + jnp.where(
        high > 0, jnp.where(alive, 6, 4), jnp.where(alive, 0, 2))

    def build_one(c):
        rows = pl.ds(c * 128, 128)
        row = rcv[pl.ds(c, 1), :]
        hot_rows(hot_t, c, 512, 768, row)
        hot_columns(hot_s, 6, c * 128, column(snd[pl.ds(c, 1), :]))
        hot_columns(hot_r, 6, c * 128, column(row))
        code[rows, :] = column(codes[pl.ds(c, 1), :])

    def build_tile(j):
        for c in range(chunks):
            build_one(j * chunks + c)

    def lay_out_weights(s):
        full = jnp.transpose(w_in_t[s, :, 0:128].astype(F32)).astype(BF16)
        w_e2[s, 0, 0:128, :] = full
        w_e2[s, 1, 128:256, :] = full
        w_sr_t[s, 0:128, :] = w_in_t[s, :, 128:256]
        w_sr_t[s, 128:256, :] = w_in_t[s, :, 256:384]
        full = centred(w_out_full[s, :, :])
        w_o2[s, 0, 0:128, :] = full
        w_o2[s, 1, 128:256, :] = full

    def project_owned(s):
        for h in range(2):
            proj = mm_t(x[h * 512 : (h + 1) * 512, :], w_sr_t[s, :, :]).astype(BF16)
            tab_s[h, 0:512, :] = proj[:, 0:128]
            tab_r[h, 0:512, :] = proj[:, 128:256]

    def gather(hots, tab, rows, groups, table_rows):
        return mm(beside(*[hots[g, rows, :] for g in groups]),
                  beside(tab[0, table_rows, :], tab[1, table_rows, :]))

    def with_picked(lin, from_s, from_r, rows):
        held = code[rows, :]
        lin = lin + pick_half(from_s, (held & 1) > 0)
        return lin + pick_half(from_r, held >= 4)

    def owned_part(s, j):
        rows = pl.ds(j * tile, tile)
        owned_rows = pl.ds(0, 512)
        pair = beside(e[pl.ds(j * tile, half), :], e[pl.ds(j * tile + half, half), :])
        lin = mm(pair, beside(w_e2[s, 0, :, :], w_e2[s, 1, :, :]))
        lin = below(lin[:, 0:128], lin[:, 128:256])
        from_s = gather(hot_s, tab_s, rows, range(4), owned_rows)
        from_r = gather(hot_r, tab_r, rows, range(4), owned_rows)
        acc[rows, :] = with_picked(lin, from_s, from_r, rows)

    build_tile(0)
    build_tile(1)
    for copy in weight_copies:
        copy.wait()
    lay_out_weights(0)
    project_owned(0)
    for j in range(tiles):
        if j + 2 < tiles:
            build_tile(j + 2)
        owned_part(0, j)

    def layer_step(s, carry):
        fwd_copy(s).wait_recv()
        for h in range(2):
            held = below(halo[s, 2 * h, :, :], halo[s, 2 * h + 1, :, :])
            proj = mm_t(held, w_sr_t[s, :, :]).astype(BF16)
            tab_s[h, 512:768, :] = proj[:, 0:128]
            tab_r[h, 512:768, :] = proj[:, 128:256]

        halo_rows = pl.ds(512, 256)

        def hidden_of(j):
            rows = pl.ds(j * tile, tile)
            from_s = gather(hot_s, tab_s, rows, (4, 5), halo_rows)
            from_r = gather(hot_r, tab_r, rows, (4, 5), halo_rows)
            lin = with_picked(acc[rows, :], from_s, from_r, rows)
            return jnp.maximum(lin, 0.0).astype(BF16)

        def message_of(j, hidden):
            rows = pl.ds(j * tile, tile)
            pair = beside(hidden[0:half, :], hidden[half:tile, :])
            out = mm(pair, beside(w_o2[s, 0, :, :], w_o2[s, 1, :, :]))
            out = norm_centred(below(out[:, 0:128], out[:, 128:256]))
            held = code[rows, :]
            msg2[0, rows, :] = jnp.where(held < 2, out, 0.0).astype(BF16)
            msg2[1, rows, :] = jnp.where(held >= 6, out, 0.0).astype(BF16)

        hidden = hidden_of(0)
        for j in range(tiles):
            later = hidden_of(j + 1) if j + 1 < tiles else None
            message_of(j, hidden)
            hidden = later

        def scatter(row_from, row_to):
            return mm(beside(*[hot_t[c, row_from:row_to, :] for c in range(edges // 128)]),
                      beside(msg2[0, 0:edges, :], msg2[1, 0:edges, :])).astype(BF16)

        for i in range(2):
            sums = scatter(512 + i * 128, 640 + i * 128)
            ret_buf[s, i, :, :] = sums[:, 0:128]
            ret_buf[s, 2 + i, :, :] = sums[:, 128:256]
        for k in range(4):
            ret_copy(s, k).start()

        @pl.when(s == 0)
        def _():
            for k in range(4):
                row = sidx[pl.ds(k, 1), :]
                hot_rows(pick_t, k, 0, 512, jnp.where(row < 0, -1, row & 511))
                wide = column(row)
                wide = jnp.where(wide < 0, -2, wide)
                for i in range(8):
                    part = wide[i * 16 : (i + 1) * 16, :]
                    for g in range(4):
                        other = jnp.broadcast_to(sidx[pl.ds(g, 1), :], (16, 128))
                        same[g, pl.ds(k * 128 + i * 16, 16), :] = jnp.where(
                            part == other, 1.0, 0.0).astype(BF16)

            def build_owned(c, carry):
                hot_rows(hot_t, c, 0, 512, rcv[pl.ds(c, 1), :])
                return carry

            lax.fori_loop(0, edges // 128, build_owned, 0)
            for layer in range(LAYERS):
                n_out_mid[layer, :, :] = centred(n_out_full[layer, :, :])
                if layer > 0:
                    lay_out_weights(layer)

        for i in range(4):
            owned = scatter(i * 128, (i + 1) * 128)
            own_buf[s, i * 128 : (i + 1) * 128, :] = owned[:, 0:128]
            own_buf[s, 512 + i * 128 : 512 + (i + 1) * 128, :] = owned[:, 128:256]
        own_copy(s).start()

        for j in range(tiles):
            rows = pl.ds(j * tile, tile)
            message = msg2[0, rows, :].astype(F32) + msg2[1, rows, :].astype(F32)
            e[rows, :] = (e[rows, :].astype(F32) + message).astype(BF16)

        fwd_copy(s).wait_send()

        high = pick_hi[...] > 0
        places = beside(*[pick_t[k, :, :] for k in range(4)])

        def returned_sum(source):
            block = below(*[ret[s, source, k, :, :] for k in range(4)]).astype(F32)
            both = beside(jnp.where(high, 0.0, block), jnp.where(high, block, 0.0))
            both = both.astype(BF16)
            return below(mm(places[0:256, :], both), mm(places[256:512, :], both))

        def returned_sent(source):
            block = below(*[ret[s, source, k, :, :] for k in range(4)])
            alike = beside(*[same[g, :, :] for g in range(4)])
            return below(mm(alike[0:256, :], block), mm(alike[256:512, :], block))

        own_copy(s).wait_recv()
        for h in range(2):
            rows = pl.ds(h * 512, 512)
            own_sum[rows, :] = own_buf[s, rows, :].astype(F32) + own_peer[s, rows, :].astype(F32)
            own_lin[rows, :] = mm_t(x[rows, :], n_in_t[s, :, 0:128])

        @pl.when(s < LAYERS - 1)
        def _():
            here = picked(x[0:512, :], x[512:1024, :]).astype(BF16)
            sent_x[...] = here
            sent_lin[...] = mm_t(here, n_in_t[s, :, 0:128])
            sent_sum[...] = picked(own_buf[s, 0:512, :], own_buf[s, 512:1024, :]) + picked(
                own_peer[s, 0:512, :], own_peer[s, 512:1024, :])

        for k in range(4):
            ret_copy(s, k).wait_recv()
            relay_copy(s, k).start()
        ret_copy(s).wait_send()
        own_copy(s).wait_send()
        sent_back[...] = returned_sent(t)
        back_sum[...] = returned_sum(t)
        relay_copy(s).wait_recv()

        @pl.when(s < LAYERS - 1)
        def _():
            back = sent_back[...] + returned_sent(1 - t)
            total = (sent_sum[...] + back).astype(BF16)
            lin = sent_lin[...] + mm_t(total, n_in_t[s, :, 128:256])
            hidden = jnp.maximum(lin, 0.0).astype(BF16)
            update = norm_centred(mm(hidden, n_out_mid[s, :, :]))
            fill_fwd(s + 1, (sent_x[...].astype(F32) + update).astype(BF16))
            for k in range(4):
                fwd_copy(s + 1, k).start()

        back = back_sum[...] + returned_sum(1 - t)
        for h in range(2):
            rows = pl.ds(h * 512, 512)
            total = (own_sum[rows, :] + back[:, h * 128 : (h + 1) * 128]).astype(BF16)
            lin = own_lin[rows, :] + mm_t(total, n_in_t[s, :, 128:256])
            hidden = jnp.maximum(lin, 0.0).astype(BF16)
            update = norm_centred(mm(hidden, n_out_mid[s, :, :]))
            x[rows, :] = (x[rows, :].astype(F32) + update).astype(BF16)

        @pl.when(s < LAYERS - 1)
        def _():
            project_owned(s + 1)
            for j in range(tiles):
                owned_part(s + 1, j)

        relay_copy(s).wait_send()
        return carry

    lax.fori_loop(0, LAYERS, layer_step, 0)


def copy_out(x, e, x_out, e_out, sem):
    copies = [
        pltpu.make_async_copy(e, e_out, sem.at[0]),
        pltpu.make_async_copy(x, x_out, sem.at[1]),
    ]
    for copy in copies:
        copy.start()
    for copy in copies:
        copy.wait()


def local(
    doms,
    node_latent, edge_latent, edge_sender, edge_receiver, edge_count, send_index,
    edge_in, edge_out, node_in, node_out,
):
    edges = edge_latent.shape[0]
    tile = min(512, edges)
    tiles = edges // tile
    vmem = pl.BlockSpec(memory_space=pltpu.VMEM)
    hbm = pl.BlockSpec(memory_space=pltpu.HBM)
    dma = pltpu.SemaphoreType.DMA
    packed = (edges // 128, 128)
    scratch = [
        pltpu.VMEM(packed, I32),
        pltpu.VMEM(packed, I32),
        pltpu.VMEM(packed, I32),
        pltpu.SMEM((1, 1), I32),
        pltpu.VMEM((4, 128), I32),
        pltpu.VMEM((LAYERS, 64, 384), BF16),
        pltpu.VMEM((LAYERS, 64, 128), BF16),
        pltpu.VMEM((LAYERS, 64, 256), BF16),
        pltpu.VMEM((LAYERS, 64, 128), BF16),
        pltpu.VMEM((6, edges, 128), BF16),
        pltpu.VMEM((6, edges, 128), BF16),
        pltpu.VMEM((edges // 128, 768, 128), BF16),
        pltpu.VMEM((edges, 128), I32),
        pltpu.VMEM((edges, 128), F32),
        pltpu.VMEM((2, edges, 128), BF16),
        pltpu.VMEM((4, 512, 128), BF16),
        pltpu.VMEM((4, 512, 128), BF16),
        pltpu.VMEM((512, 128), I32),
        pltpu.VMEM((2, 768, 128), BF16),
        pltpu.VMEM((2, 768, 128), BF16),
        pltpu.VMEM((512, 256), F32),
        pltpu.VMEM((1024, 128), F32),
        pltpu.VMEM((1024, 128), F32),
        pltpu.VMEM((4, 512, 128), BF16),
        pltpu.VMEM((512, 128), BF16),
        pltpu.VMEM((512, 128), F32),
        pltpu.VMEM((512, 128), F32),
        pltpu.VMEM((512, 128), F32),
        pltpu.VMEM((LAYERS, 128, 384), BF16),
        pltpu.VMEM((LAYERS, 128, 256), BF16),
        pltpu.VMEM((LAYERS, 128, 128), BF16),
        pltpu.VMEM((LAYERS, 128, 128), BF16),
        pltpu.VMEM((LAYERS, 128, 128), BF16),
        pltpu.VMEM((LAYERS, 256, 128), BF16),
        pltpu.VMEM((LAYERS, 2, 256, 128), BF16),
        pltpu.VMEM((LAYERS, 2, 256, 128), BF16),
        pltpu.VMEM((LAYERS, 4, 128, 128), BF16),
        pltpu.VMEM((LAYERS, 4, 128, 128), BF16),
        pltpu.VMEM((LAYERS, 4, 128, 128), BF16),
        pltpu.VMEM((LAYERS, 2, 4, 128, 128), BF16),
        pltpu.VMEM((LAYERS, 1024, 128), BF16),
        pltpu.VMEM((LAYERS, 1024, 128), BF16),
        dma((10,)), dma((4,)), dma((4,)), dma((LAYERS,)), dma((LAYERS, 4)),
        dma((LAYERS,)), dma((LAYERS,)),
    ]
    nodes, edges_now = pl.pallas_call(
        functools.partial(kernel, doms, tile),
        out_shape=(
            pltpu.VMEM(node_latent.shape, BF16),
            pltpu.VMEM(edge_latent.shape, BF16),
        ),
        in_specs=[hbm] * 10,
        out_specs=(vmem, vmem),
        scratch_shapes=scratch,
        compiler_params=pltpu.CompilerParams(
            collective_id=0, has_side_effects=True, vmem_limit_bytes=65700000,
        ),
    )(
        node_latent, edge_latent,
        edge_sender.reshape(-1, 128), edge_receiver.reshape(-1, 128),
        edge_count.reshape(1, 1), send_index.reshape(4, 128),
        jnp.swapaxes(edge_in, 1, 2), edge_out, jnp.swapaxes(node_in, 1, 2), node_out,
    )
    anywhere = pl.BlockSpec(memory_space=pl.ANY)
    return pl.pallas_call(
        copy_out,
        out_shape=(
            jax.ShapeDtypeStruct(node_latent.shape, BF16),
            jax.ShapeDtypeStruct(edge_latent.shape, BF16),
        ),
        in_specs=[anywhere, anywhere],
        out_specs=(anywhere, anywhere),
        scratch_shapes=[dma((2,))],
        compiler_params=pltpu.CompilerParams(vmem_limit_bytes=8 << 20),
    )(nodes, edges_now)


def solution(mesh):
    return jax.shard_map(
        functools.partial(local, mesh.shape["dom"]),
        mesh=mesh,
        in_specs=(
            P("dom", None),
            P(("dom", "tp"), None),
            P(("dom", "tp")),
            P(("dom", "tp")),
            P(("dom", "tp")),
            P("dom", None, None),
            P(None, None, "tp"),
            P(None, "tp", None),
            P(None, None, "tp"),
            P(None, "tp", None),
        ),
        out_specs=(P("dom", None), P(("dom", "tp"), None)),
        check_vma=False,
    )
```

```python
import functools

import jax
import jax.numpy as jnp
from jax import lax
from jax.experimental import pallas as pl
from jax.experimental.pallas import tpu as pltpu
from jax.sharding import PartitionSpec as P

LAYERS = 3
OFFSETS = (1, -1, 2, -2)
NORM_FLOOR = 0.25
MESH = pl.DeviceIdType.MESH
F32 = jnp.float32
BF16 = jnp.bfloat16
I16 = jnp.int16
I32 = jnp.int32


def mm(a, b):
    return jnp.dot(a, b, preferred_element_type=F32)


def mm_t(a, b):
    return lax.dot_general(a, b, (((1,), (1,)), ((), ())), preferred_element_type=F32)


def beside(*parts):
    return jnp.concatenate(parts, axis=1)


def below(*parts):
    return jnp.concatenate(parts, axis=0)


def norm_centred(values):
    spread = jnp.sum(values * values, axis=-1, keepdims=True) * (1.0 / 128.0)
    return values * lax.rsqrt(spread + NORM_FLOOR)


def centred(weights):
    wide = weights.astype(F32)
    return (wide - jnp.mean(wide, axis=-1, keepdims=True)).astype(BF16)


def hot(match):
    return jnp.where(match, jnp.ones((), BF16), jnp.zeros((), BF16))


def column(row):
    return jnp.transpose(jnp.broadcast_to(row, (128, 128)))


def pick_half(both, high):
    return jnp.where(high, both[:, 128:], both[:, :128])


def kernel(
    doms, tile,
    x_hbm, e_hbm, snd_hbm, rcv_hbm, cnt_hbm, sidx_hbm, w_in_hbm, w_out_hbm, n_in_hbm, n_out_hbm,
    x, e,
    snd, rcv, codes, cnt, sidx, w_in, w_out, n_in, n_out,
    hot_s, hot_r, hot_t, code, acc, msg2,
    pick, pick_t, pick_hi, tab_s, tab_r, back_sum, own_sum, own_lin,
    same, sent_x, sent_lin, sent_sum, sent_back,
    w_in_t, n_in_t, w_out_full, n_out_full, n_out_mid, w_sr_t, w_e2, w_o2,
    fwd_buf, halo, ret_buf, ret, own_buf, own_peer,
    in_sem, send_sem, w_recv, fwd_recv, ret_recv, rel_recv, own_recv,
):
    p = lax.axis_index("dom")
    t = lax.axis_index("tp")
    peer = (p, 1 - t)
    to = [(lax.rem(p + o + doms, doms), 1 - t) for o in OFFSETS]
    back = [(lax.rem(p - o + doms, doms), 1 - t) for o in OFFSETS]
    edges = e.shape[0]
    tiles = edges // tile
    half = tile // 2
    chunks = tile // 128

    barrier = pltpu.get_barrier_semaphore()
    for other in to + [peer]:
        pl.semaphore_signal(barrier, inc=1, device_id=other, device_id_type=MESH)

    loads = [
        pltpu.make_async_copy(src, dst, in_sem.at[i])
        for i, (src, dst) in enumerate([
            (sidx_hbm, sidx), (x_hbm, x), (w_in_hbm, w_in), (w_out_hbm, w_out),
            (n_in_hbm, n_in), (n_out_hbm, n_out), (snd_hbm, snd), (rcv_hbm, rcv),
            (cnt_hbm, cnt), (e_hbm, e)])
    ]
    for copy in loads:
        copy.start()

    def remote(src, dst, send, recv, device):
        return pltpu.make_async_remote_copy(
            src_ref=src, dst_ref=dst, send_sem=send, recv_sem=recv,
            device_id=device, device_id_type=MESH,
        )

    def fwd_copy(layer, *k):
        return remote(fwd_buf.at[(layer, *k)], halo.at[(layer, *k)],
                      send_sem.at[0], fwd_recv.at[layer], to[k[0] if k else 0])

    def ret_copy(layer, *k):
        return remote(ret_buf.at[(layer, *k)], ret.at[(layer, 1 - t, *k)],
                      send_sem.at[1], ret_recv.at[layer, k[0] if k else 0], back[k[0] if k else 0])

    def relay_copy(layer, *k):
        return remote(ret.at[(layer, t, *k)], ret.at[(layer, t, *k)],
                      send_sem.at[2], rel_recv.at[layer], peer)

    def own_copy(layer):
        return remote(own_buf.at[layer], own_peer.at[layer],
                      send_sem.at[3], own_recv.at[layer], peer)

    rows64 = pl.ds(pl.multiple_of(t * 64, 64), 64)
    weight_copies = [
        remote(src, dst.at[:, rows64, :], in_sem.at[2 + i], w_recv.at[i], peer)
        for i, (src, dst) in enumerate(
            [(w_in, w_in_t), (w_out, w_out_full), (n_in, n_in_t), (n_out, n_out_full)])
    ]

    lane = lax.broadcasted_iota(I32, (128, 128), 1)
    sub = lax.broadcasted_iota(I32, (128, 128), 0)
    sub16 = lax.broadcasted_iota(I32, (16, 128), 0).astype(I16)
    lane_of = [lax.broadcasted_iota(I32, (16, 128), 1) + g * 128 for g in range(6)]

    def hot_columns(ref, groups, start, low):
        for i in range(8):
            part = low[i * 16 : (i + 1) * 16, :]
            for g in range(groups):
                ref[g, pl.ds(start + i * 16, 16), :] = jnp.where(
                    part == lane_of[g], 1.0, 0.0).astype(BF16)

    def hot_rows(ref, c, row_from, row_to, low_row):
        wide = jnp.broadcast_to(low_row, (16, 128)).astype(I16)
        for i in range(row_from // 16, row_to // 16):
            ref[c, i * 16 : (i + 1) * 16, :] = hot(wide - I16(i * 16) == sub16)

    w_e2[...] = jnp.zeros_like(w_e2)
    w_o2[...] = jnp.zeros_like(w_o2)

    loads[0].wait()
    loads[1].wait()
    for k in range(4):
        row = sidx[pl.ds(k, 1), :]
        wide = column(row)
        rows = pl.ds(k * 128, 128)
        low = jnp.where(wide < 0, -1, wide & 511)
        pick_hi[rows, :] = jnp.where(wide >= 512, 1, 0)
        hot_columns(pick, 4, k * 128, low)

    def picked(top, bottom):
        table = beside(top, bottom)
        parts = []
        for h in range(2):
            rows = pl.ds(h * 256, 256)
            both = mm(beside(*[pick[g, rows, :] for g in range(4)]), table)
            parts.append(pick_half(both, pick_hi[rows, :] > 0))
        return below(*parts)

    def fill_fwd(layer, rows):
        for k in range(4):
            fwd_buf[layer, k, :, :] = rows[k * 128 : (k + 1) * 128, :]

    fill_fwd(0, picked(x[0:512, :], x[512:1024, :]).astype(BF16))
    for copy in loads[2:6]:
        copy.wait()
    for src, dst in [(w_in, w_in_t), (w_out, w_out_full), (n_in, n_in_t), (n_out, n_out_full)]:
        dst[:, rows64, :] = src[...]
    pl.semaphore_wait(barrier, 5)
    for k in range(4):
        fwd_copy(0, k).start()
    for copy in weight_copies:
        copy.start()

    for copy in loads[6:]:
        copy.wait()
    live = cnt[0, 0]

    def split(row):
        own = row < 1024
        low = jnp.where(own, row & 511, 512 + (row & 255))
        high = jnp.where(own, row >> 9, (row >> 8) & 1)
        return low, high

    low, high_s = split(snd[...])
    snd[...] = low
    low, high = split(rcv[...])
    rcv[...] = low
    slot = (lax.broadcasted_iota(I32, snd.shape, 0) * 128
            + lax.broadcasted_iota(I32, snd.shape, 1))
    alive = slot < live
    codes[...] = high_s + jnp.where(
        high > 0, jnp.where(alive, 6, 4), jnp.where(alive, 0, 2))

    def build_one(c):
        rows = pl.ds(c * 128, 128)
        row = rcv[pl.ds(c, 1), :]
        hot_rows(hot_t, c, 512, 768, row)
        hot_columns(hot_s, 6, c * 128, column(snd[pl.ds(c, 1), :]))
        hot_columns(hot_r, 6, c * 128, column(row))
        code[rows, :] = column(codes[pl.ds(c, 1), :])

    def build_tile(j):
        for c in range(chunks):
            build_one(j * chunks + c)

    def lay_out_weights(s):
        full = jnp.transpose(w_in_t[s, :, 0:128].astype(F32)).astype(BF16)
        w_e2[s, 0, 0:128, :] = full
        w_e2[s, 1, 128:256, :] = full
        w_sr_t[s, 0:128, :] = w_in_t[s, :, 128:256]
        w_sr_t[s, 128:256, :] = w_in_t[s, :, 256:384]
        full = centred(w_out_full[s, :, :])
        w_o2[s, 0, 0:128, :] = full
        w_o2[s, 1, 128:256, :] = full

    def project_owned(s):
        for h in range(2):
            proj = mm_t(x[h * 512 : (h + 1) * 512, :], w_sr_t[s, :, :]).astype(BF16)
            tab_s[h, 0:512, :] = proj[:, 0:128]
            tab_r[h, 0:512, :] = proj[:, 128:256]

    def gather(hots, tab, rows, groups, table_rows):
        return mm(beside(*[hots[g, rows, :] for g in groups]),
                  beside(tab[0, table_rows, :], tab[1, table_rows, :]))

    def with_picked(lin, from_s, from_r, rows):
        held = code[rows, :]
        lin = lin + pick_half(from_s, (held & 1) > 0)
        return lin + pick_half(from_r, held >= 4)

    def owned_part(s, j):
        rows = pl.ds(j * tile, tile)
        owned_rows = pl.ds(0, 512)
        pair = beside(e[pl.ds(j * tile, half), :], e[pl.ds(j * tile + half, half), :])
        lin = mm(pair, beside(w_e2[s, 0, :, :], w_e2[s, 1, :, :]))
        lin = below(lin[:, 0:128], lin[:, 128:256])
        from_s = gather(hot_s, tab_s, rows, range(4), owned_rows)
        from_r = gather(hot_r, tab_r, rows, range(4), owned_rows)
        acc[rows, :] = with_picked(lin, from_s, from_r, rows)

    build_tile(0)
    build_tile(1)
    for copy in weight_copies:
        copy.wait()
    lay_out_weights(0)
    project_owned(0)
    for j in range(tiles):
        if j + 2 < tiles:
            build_tile(j + 2)
        owned_part(0, j)

    def layer_step(s, carry):
        fwd_copy(s).wait_recv()
        for h in range(2):
            held = below(halo[s, 2 * h, :, :], halo[s, 2 * h + 1, :, :])
            proj = mm_t(held, w_sr_t[s, :, :]).astype(BF16)
            tab_s[h, 512:768, :] = proj[:, 0:128]
            tab_r[h, 512:768, :] = proj[:, 128:256]

        halo_rows = pl.ds(512, 256)

        def hidden_of(j):
            rows = pl.ds(j * tile, tile)
            from_s = gather(hot_s, tab_s, rows, (4, 5), halo_rows)
            from_r = gather(hot_r, tab_r, rows, (4, 5), halo_rows)
            lin = with_picked(acc[rows, :], from_s, from_r, rows)
            return jnp.maximum(lin, 0.0).astype(BF16)

        def message_of(j, hidden):
            rows = pl.ds(j * tile, tile)
            pair = beside(hidden[0:half, :], hidden[half:tile, :])
            out = mm(pair, beside(w_o2[s, 0, :, :], w_o2[s, 1, :, :]))
            out = norm_centred(below(out[:, 0:128], out[:, 128:256]))
            held = code[rows, :]
            msg2[0, rows, :] = jnp.where(held < 2, out, 0.0).astype(BF16)
            msg2[1, rows, :] = jnp.where(held >= 6, out, 0.0).astype(BF16)

        hidden = hidden_of(0)
        for j in range(tiles):
            later = hidden_of(j + 1) if j + 1 < tiles else None
            message_of(j, hidden)
            hidden = later

        def scatter(row_from, row_to):
            return mm(beside(*[hot_t[c, row_from:row_to, :] for c in range(edges // 128)]),
                      beside(msg2[0, 0:edges, :], msg2[1, 0:edges, :])).astype(BF16)

        for i in range(2):
            sums = scatter(512 + i * 128, 640 + i * 128)
            ret_buf[s, i, :, :] = sums[:, 0:128]
            ret_buf[s, 2 + i, :, :] = sums[:, 128:256]
        for k in range(4):
            ret_copy(s, k).start()

        @pl.when(s == 0)
        def _():
            for k in range(4):
                row = sidx[pl.ds(k, 1), :]
                hot_rows(pick_t, k, 0, 512, jnp.where(row < 0, -1, row & 511))
                wide = column(row)
                wide = jnp.where(wide < 0, -2, wide)
                for i in range(8):
                    part = wide[i * 16 : (i + 1) * 16, :]
                    for g in range(4):
                        other = jnp.broadcast_to(sidx[pl.ds(g, 1), :], (16, 128))
                        same[g, pl.ds(k * 128 + i * 16, 16), :] = jnp.where(
                            part == other, 1.0, 0.0).astype(BF16)

            def build_owned(c, carry):
                hot_rows(hot_t, c, 0, 512, rcv[pl.ds(c, 1), :])
                return carry

            lax.fori_loop(0, edges // 128, build_owned, 0)
            for layer in range(LAYERS):
                n_out_mid[layer, :, :] = centred(n_out_full[layer, :, :])
                if layer > 0:
                    lay_out_weights(layer)

        for i in range(4):
            owned = scatter(i * 128, (i + 1) * 128)
            own_buf[s, i * 128 : (i + 1) * 128, :] = owned[:, 0:128]
            own_buf[s, 512 + i * 128 : 512 + (i + 1) * 128, :] = owned[:, 128:256]
        own_copy(s).start()

        for j in range(tiles):
            rows = pl.ds(j * tile, tile)
            message = msg2[0, rows, :].astype(F32) + msg2[1, rows, :].astype(F32)
            e[rows, :] = (e[rows, :].astype(F32) + message).astype(BF16)

        fwd_copy(s).wait_send()

        high = pick_hi[...] > 0
        places = beside(*[pick_t[k, :, :] for k in range(4)])

        def returned_sum(source):
            block = below(*[ret[s, source, k, :, :] for k in range(4)]).astype(F32)
            both = beside(jnp.where(high, 0.0, block), jnp.where(high, block, 0.0))
            both = both.astype(BF16)
            return below(mm(places[0:256, :], both), mm(places[256:512, :], both))

        def returned_sent(source):
            block = below(*[ret[s, source, k, :, :] for k in range(4)])
            alike = beside(*[same[g, :, :] for g in range(4)])
            return below(mm(alike[0:256, :], block), mm(alike[256:512, :], block))

        own_copy(s).wait_recv()
        for h in range(2):
            rows = pl.ds(h * 512, 512)
            own_sum[rows, :] = own_buf[s, rows, :].astype(F32) + own_peer[s, rows, :].astype(F32)
            own_lin[rows, :] = mm_t(x[rows, :], n_in_t[s, :, 0:128])

        @pl.when(s < LAYERS - 1)
        def _():
            here = picked(x[0:512, :], x[512:1024, :]).astype(BF16)
            sent_x[...] = here
            sent_lin[...] = mm_t(here, n_in_t[s, :, 0:128])
            sent_sum[...] = picked(own_buf[s, 0:512, :], own_buf[s, 512:1024, :]) + picked(
                own_peer[s, 0:512, :], own_peer[s, 512:1024, :])

        for k in range(4):
            ret_copy(s, k).wait_recv()
            relay_copy(s, k).start()
        ret_copy(s).wait_send()
        own_copy(s).wait_send()
        sent_back[...] = returned_sent(t)
        back_sum[...] = returned_sum(t)
        relay_copy(s).wait_recv()

        @pl.when(s < LAYERS - 1)
        def _():
            back = sent_back[...] + returned_sent(1 - t)
            total = (sent_sum[...] + back).astype(BF16)
            lin = sent_lin[...] + mm_t(total, n_in_t[s, :, 128:256])
            hidden = jnp.maximum(lin, 0.0).astype(BF16)
            update = norm_centred(mm(hidden, n_out_mid[s, :, :]))
            fill_fwd(s + 1, (sent_x[...].astype(F32) + update).astype(BF16))
            for k in range(4):
                fwd_copy(s + 1, k).start()

        back = back_sum[...] + returned_sum(1 - t)
        for h in range(2):
            rows = pl.ds(h * 512, 512)
            total = (own_sum[rows, :] + back[:, h * 128 : (h + 1) * 128]).astype(BF16)
            lin = own_lin[rows, :] + mm_t(total, n_in_t[s, :, 128:256])
            hidden = jnp.maximum(lin, 0.0).astype(BF16)
            update = norm_centred(mm(hidden, n_out_mid[s, :, :]))
            x[rows, :] = (x[rows, :].astype(F32) + update).astype(BF16)

        @pl.when(s < LAYERS - 1)
        def _():
            project_owned(s + 1)
            for j in range(tiles):
                owned_part(s + 1, j)

        relay_copy(s).wait_send()
        return carry

    lax.fori_loop(0, LAYERS, layer_step, 0)


def copy_out(x, e, x_out, e_out, sem):
    copies = [
        pltpu.make_async_copy(e, e_out, sem.at[0]),
        pltpu.make_async_copy(x, x_out, sem.at[1]),
    ]
    for copy in copies:
        copy.start()
    for copy in copies:
        copy.wait()


def local(
    doms,
    node_latent, edge_latent, edge_sender, edge_receiver, edge_count, send_index,
    edge_in, edge_out, node_in, node_out,
):
    edges = edge_latent.shape[0]
    tile = min(512, edges)
    tiles = edges // tile
    vmem = pl.BlockSpec(memory_space=pltpu.VMEM)
    hbm = pl.BlockSpec(memory_space=pltpu.HBM)
    dma = pltpu.SemaphoreType.DMA
    packed = (edges // 128, 128)
    scratch = [
        pltpu.VMEM(packed, I32),
        pltpu.VMEM(packed, I32),
        pltpu.VMEM(packed, I32),
        pltpu.SMEM((1, 1), I32),
        pltpu.VMEM((4, 128), I32),
        pltpu.VMEM((LAYERS, 64, 384), BF16),
        pltpu.VMEM((LAYERS, 64, 128), BF16),
        pltpu.VMEM((LAYERS, 64, 256), BF16),
        pltpu.VMEM((LAYERS, 64, 128), BF16),
        pltpu.VMEM((6, edges, 128), BF16),
        pltpu.VMEM((6, edges, 128), BF16),
        pltpu.VMEM((edges // 128, 768, 128), BF16),
        pltpu.VMEM((edges, 128), I32),
        pltpu.VMEM((edges, 128), F32),
        pltpu.VMEM((2, edges, 128), BF16),
        pltpu.VMEM((4, 512, 128), BF16),
        pltpu.VMEM((4, 512, 128), BF16),
        pltpu.VMEM((512, 128), I32),
        pltpu.VMEM((2, 768, 128), BF16),
        pltpu.VMEM((2, 768, 128), BF16),
        pltpu.VMEM((512, 256), F32),
        pltpu.VMEM((1024, 128), F32),
        pltpu.VMEM((1024, 128), F32),
        pltpu.VMEM((4, 512, 128), BF16),
        pltpu.VMEM((512, 128), BF16),
        pltpu.VMEM((512, 128), F32),
        pltpu.VMEM((512, 128), F32),
        pltpu.VMEM((512, 128), F32),
        pltpu.VMEM((LAYERS, 128, 384), BF16),
        pltpu.VMEM((LAYERS, 128, 256), BF16),
        pltpu.VMEM((LAYERS, 128, 128), BF16),
        pltpu.VMEM((LAYERS, 128, 128), BF16),
        pltpu.VMEM((LAYERS, 128, 128), BF16),
        pltpu.VMEM((LAYERS, 256, 128), BF16),
        pltpu.VMEM((LAYERS, 2, 256, 128), BF16),
        pltpu.VMEM((LAYERS, 2, 256, 128), BF16),
        pltpu.VMEM((LAYERS, 4, 128, 128), BF16),
        pltpu.VMEM((LAYERS, 4, 128, 128), BF16),
        pltpu.VMEM((LAYERS, 4, 128, 128), BF16),
        pltpu.VMEM((LAYERS, 2, 4, 128, 128), BF16),
        pltpu.VMEM((LAYERS, 1024, 128), BF16),
        pltpu.VMEM((LAYERS, 1024, 128), BF16),
        dma((10,)), dma((4,)), dma((4,)), dma((LAYERS,)), dma((LAYERS, 4)),
        dma((LAYERS,)), dma((LAYERS,)),
    ]
    nodes, edges_now = pl.pallas_call(
        functools.partial(kernel, doms, tile),
        out_shape=(
            pltpu.VMEM(node_latent.shape, BF16),
            pltpu.VMEM(edge_latent.shape, BF16),
        ),
        in_specs=[hbm] * 10,
        out_specs=(vmem, vmem),
        scratch_shapes=scratch,
        compiler_params=pltpu.CompilerParams(
            collective_id=0, has_side_effects=True, vmem_limit_bytes=65700000,
        ),
    )(
        node_latent, edge_latent,
        edge_sender.reshape(-1, 128), edge_receiver.reshape(-1, 128),
        edge_count.reshape(1, 1), send_index.reshape(4, 128),
        jnp.swapaxes(edge_in, 1, 2), edge_out, jnp.swapaxes(node_in, 1, 2), node_out,
    )
    anywhere = pl.BlockSpec(memory_space=pl.ANY)
    return pl.pallas_call(
        copy_out,
        out_shape=(
            jax.ShapeDtypeStruct(node_latent.shape, BF16),
            jax.ShapeDtypeStruct(edge_latent.shape, BF16),
        ),
        in_specs=[anywhere, anywhere],
        out_specs=(anywhere, anywhere),
        scratch_shapes=[dma((2,))],
        compiler_params=pltpu.CompilerParams(vmem_limit_bytes=8 << 20),
    )(nodes, edges_now)


def solution(mesh):
    return jax.shard_map(
        functools.partial(local, mesh.shape["dom"]),
        mesh=mesh,
        in_specs=(
            P("dom", None),
            P(("dom", "tp"), None),
            P(("dom", "tp")),
            P(("dom", "tp")),
            P(("dom", "tp")),
            P("dom", None, None),
            P(None, None, "tp"),
            P(None, "tp", None),
            P(None, None, "tp"),
            P(None, "tp", None),
        ),
        out_specs=(P("dom", None), P(("dom", "tp"), None)),
        check_vma=False,
    )
```
